32 devices in a mesh: fsdp: 8 (over y, x, core), ctx: 4 (over z).
Axes of the slice: x: 2, y: 2, z: 4, core: 2. Of those that a mesh axis runs over, the one named last changes fastest.
Arguments:
- tokens: bfloat16 [8, 1024, 1024], P('fsdp', 'ctx'), may hold values from -6 to 6
- segments: int32 [8, 1024], P('fsdp', 'ctx'), may hold values from 0 to 7, never falling along the last dimension, each value on 1 to 512 neighbouring positions
- cotangent: bfloat16 [8, 1024, 1024], P('fsdp', 'ctx'), may hold values from -6 to 6
- attn_gain: bfloat16 [1024], P('fsdp'), may hold values from 0.5 to 1.5
- w_query: bfloat16 [1024, 2048], P('fsdp'), may hold values from -0.1875 to 0.1875
- key_matrix: bfloat16 [1024, 1024], P('fsdp'), may hold values from -0.1875 to 0.1875
- value_matrix: bfloat16 [1024, 1024], P('fsdp'), may hold values from -0.1875 to 0.1875
- w_out: bfloat16 [2048, 1024], P('fsdp'), may hold values from -1 to 1
- query_gain: bfloat16 [128], replicated, may hold values from 0.099609375 to 1.8984375
- key_gain: bfloat16 [128], replicated, may hold values from 0.099609375 to 1.8984375
- ffn_gain: bfloat16 [1024], P('fsdp'), may hold values from 0.5 to 1.5
- w_gate: bfloat16 [1024, 3072], P('fsdp'), may hold values from -0.1875 to 0.1875
- w_up: bfloat16 [1024, 3072], P('fsdp'), may hold values from -0.1875 to 0.1875
- w_down: bfloat16 [3072, 1024], P('fsdp'), may hold values from -0.109375 to 0.109375
Outputs:
- output: bfloat16 [8, 1024, 1024], P('fsdp', 'ctx')
- input_grad: float32 [8, 1024, 1024], P('fsdp', 'ctx')
- attn_gain_grad: float32 [1024], P('fsdp')
- w_query_grad: float32 [1024, 2048], P('fsdp')
- w_key_grad: float32 [1024, 1024], P('fsdp')
- w_value_grad: float32 [1024, 1024], P('fsdp')
- w_out_grad: float32 [2048, 1024], P('fsdp')
- query_gain_grad: float32 [128], replicated
- key_gain_grad: float32 [128], replicated
- ffn_gain_grad: float32 [1024], P('fsdp')
- w_gate_grad: float32 [1024, 3072], P('fsdp')
- w_up_grad: float32 [1024, 3072], P('fsdp')
- w_down_grad: float32 [3072, 1024], P('fsdp')
The draws below stay inside these ranges and needn't reach their ends.
Inputs may be any that keep to these rules, and one draw needn't show every extreme that they name: `segments`: along each sequence the segment numbers never fall; each number names one document of 1 to 512 tokens, and one document has exactly 512.
All inputs are finite; a program needn't handle non-finite values.
Results may differ from the reference program's by a relative error of at most 0.019.
Values may be sent and summed in bfloat16 or wider, within the bound.
No kernel may reach another device: no remote copies, remote signals or barrier semaphores. Data moves between devices by JAX's collectives and lax.ppermute only.
A program may use at most 192 MiB of HBM per device.

```python
import math
import jax
import jax.numpy as jnp
import numpy as np
from jax import lax

MODEL_WIDTH = 1024
QUERY_HEAD_COUNT = 16
KEY_VALUE_HEADS = 8
HEAD_SIZE = 128
FF = 3072
LEN = 1024
SEQS = 8


def block_levels(key, shape, cuts, low, high):
    level, own = 1.0, jax.random.fold_in(key, 6)
    for dim, shards_of in cuts:
        steps = jnp.exp(jax.random.uniform(jax.random.fold_in(own, dim), (shards_of,), jnp.float32, low / len(cuts), high / len(cuts)))
        level = level * jnp.repeat(steps, shape[dim] // shards_of).reshape([-1 if axis == dim else 1 for axis in range(len(shape))])
    return level


def profile(number_of, total, limit, skew):
    portions = [(1 << 20) // math.isqrt(grade ** skew) + 1 for grade in range(2, number_of + 1)]
    rest, counts = total - limit - (number_of - 1), [1] * (number_of - 1)
    while rest > 0:
        free = [i for i in range(number_of - 1) if counts[i] < limit]
        pool, budget = sum([portions[i] for i in free]), rest
        for i in free:
            addition = min(limit - counts[i], max(1, budget * portions[i] // pool), rest)
            counts[i] = counts[i] + addition
            rest = rest - addition
    return np.array([limit] + counts)


def ragged(own_key, count, total, most, skew):
    if count == 2:
        one = jax.random.randint(own_key, (), max(1, total - most), min(most, total - 1) + 1)
        return jnp.stack([one, total - one])
    lengths = jnp.asarray(profile(count, total, most, skew), jnp.int32)
    pairs = (count - 1) // 2
    donor, sink = lengths[1:1 + 2 * pairs:2], lengths[2:2 + 2 * pairs:2]
    slack = jnp.minimum(donor - 1, most - sink)
    passed = jax.random.randint(jax.random.fold_in(own_key, 1), (pairs,), 0, 1 << 20) % (slack + 1)
    lengths = lengths.at[1:1 + 2 * pairs:2].set(donor - passed).at[2:2 + 2 * pairs:2].set(sink + passed)
    return lengths[jax.random.permutation(jax.random.fold_in(own_key, 2), count)]


def normal_values(stream_key, dims, deviation, most, shards=(), held_as=jnp.bfloat16):
    loudness = block_levels(stream_key, dims, shards, -0.22, 0.18) if shards else 1.0
    values = jax.random.normal(stream_key, dims, jnp.float32) * deviation * loudness
    return jnp.minimum(jnp.maximum(values, -most), most).astype(held_as)


def setup_inputs(seed: int = 0) -> dict:
    arg_keys = jax.random.split(jax.random.key(seed), 15)
    tokens = normal_values(arg_keys[0], (SEQS, LEN, MODEL_WIDTH), 1.0, 6.0, ((0, 8), (1, 4)))
    segments = jax.vmap(lambda own: jnp.searchsorted(jnp.cumsum(ragged(own, max(4, LEN // 128), LEN, LEN // 2, 2)), jnp.arange(LEN), side="right"))(jax.random.split(arg_keys[1], SEQS)).reshape((SEQS, LEN)).astype(jnp.int32)
    cotangent = normal_values(arg_keys[2], (SEQS, LEN, MODEL_WIDTH), 1.0, 6.0, ((0, 8), (1, 4)))
    attn_gain = jnp.clip(1.0 + 0.1 * jax.random.normal(arg_keys[3], (MODEL_WIDTH,), jnp.float32), 0.5, 1.5).astype(jnp.bfloat16)
    w_query = normal_values(arg_keys[4], (MODEL_WIDTH, QUERY_HEAD_COUNT * HEAD_SIZE), MODEL_WIDTH ** -0.5, 0.1875, ((0, 8),))
    key_matrix = normal_values(arg_keys[5], (MODEL_WIDTH, KEY_VALUE_HEADS * HEAD_SIZE), MODEL_WIDTH ** -0.5, 0.1875, ((0, 8),))
    value_matrix = normal_values(arg_keys[6], (MODEL_WIDTH, KEY_VALUE_HEADS * HEAD_SIZE), MODEL_WIDTH ** -0.5, 0.1875, ((0, 8),))
    w_out = normal_values(arg_keys[7], (QUERY_HEAD_COUNT * HEAD_SIZE, MODEL_WIDTH), (QUERY_HEAD_COUNT * HEAD_SIZE // 64) ** -0.5, 1.0, ((0, 8),))
    query_gain = jnp.clip(1.0 + 0.18 * jax.random.normal(arg_keys[8], (HEAD_SIZE,), jnp.float32), 0.099609375, 1.8984375).astype(jnp.bfloat16)
    key_gain = jnp.clip(1.0 + 0.18 * jax.random.normal(arg_keys[9], (HEAD_SIZE,), jnp.float32), 0.099609375, 1.8984375).astype(jnp.bfloat16)
    ffn_gain = jnp.clip(1.0 + 0.1 * jax.random.normal(arg_keys[10], (MODEL_WIDTH,), jnp.float32), 0.5, 1.5).astype(jnp.bfloat16)
    w_gate = normal_values(arg_keys[11], (MODEL_WIDTH, FF), MODEL_WIDTH ** -0.5, 0.1875, ((0, 8),))
    w_up = normal_values(arg_keys[12], (MODEL_WIDTH, FF), MODEL_WIDTH ** -0.5, 0.1875, ((0, 8),))
    w_down = normal_values(arg_keys[13], (FF, MODEL_WIDTH), FF ** -0.5, 0.109375, ((0, 8),))
    return dict(tokens=tokens, segments=segments, cotangent=cotangent, attn_gain=attn_gain, w_query=w_query, key_matrix=key_matrix, value_matrix=value_matrix, w_out=w_out, query_gain=query_gain, key_gain=key_gain, ffn_gain=ffn_gain, w_gate=w_gate, w_up=w_up, w_down=w_down)


EPS = 1e-06
ROPE_BASE = 1000000.0
NEG = -1e+30
HIGH = lax.Precision.HIGHEST

@jax.custom_vjp
def low(v):
    return lax.optimization_barrier(v.astype(jnp.bfloat16)).astype(jnp.float32)

@jax.custom_vjp
def low_back(v):
    return v

def low_keep(v):
    return (low(v), None)

def low_pass(kept, grad):
    return (grad,)

def back_keep(v):
    return (v, None)

def back_low(kept, grad):
    return (low(grad),)
low.defvjp(low_keep, low_pass)
low_back.defvjp(back_keep, back_low)

def matrix_product(left, right):
    return jnp.dot(left, right, precision=HIGH)

def rms_norm(values, gain):
    return values * lax.rsqrt(lax.optimization_barrier(jnp.mean(values * values, axis=-1, keepdims=True)) + EPS) * gain

def rotate(values, cosine, sine):
    half = values.shape[-1] // 2
    first = values[..., :half]
    second = values[..., half:]
    return jnp.concatenate([first * cosine - second * sine, second * cosine + first * sine], axis=-1)

def place_of(segs):
    span_length = segs.shape[0]
    index = jnp.arange(span_length, dtype=jnp.int32)
    begins = jnp.concatenate([jnp.ones((1,), dtype=bool), segs[1:] != segs[:-1]])
    start = lax.cummax(jnp.where(begins, index, jnp.zeros_like(index)), axis=0)
    return index - start

def layer(resid, segs, attn_gain, w_query, key_matrix, value_matrix, w_out, query_gain, key_gain, ffn_gain, w_gate, w_up, w_down):
    span_length = resid.shape[0]
    head_group = QUERY_HEAD_COUNT // KEY_VALUE_HEADS
    attention_normed = low(rms_norm(resid, attn_gain))
    query_raw = low_back(matrix_product(attention_normed, w_query)).reshape(span_length, QUERY_HEAD_COUNT, HEAD_SIZE)
    key_unnormed = low_back(matrix_product(attention_normed, key_matrix)).reshape(span_length, KEY_VALUE_HEADS, HEAD_SIZE)
    value_reduced = low_back(low(matrix_product(attention_normed, value_matrix))).reshape(span_length, KEY_VALUE_HEADS, HEAD_SIZE)
    place = place_of(segs).astype(jnp.float32)
    half = HEAD_SIZE // 2
    freq = 1.0 / ROPE_BASE ** (jnp.arange(half, dtype=jnp.float32) * 2.0 / HEAD_SIZE)
    angle = place[:, None] * freq[None, :]
    cosine = jnp.cos(angle)[:, None, :]
    sine = jnp.sin(angle)[:, None, :]
    query_reduced = low(rotate(rms_norm(query_raw, query_gain), cosine, sine))
    key_low = low(rotate(rms_norm(key_unnormed, key_gain), cosine, sine))
    block_span = min(512, span_length)
    item_count = span_length // block_span
    key_index = jnp.arange(span_length, dtype=jnp.int32)
    query_block_list = query_reduced.reshape(item_count, block_span, KEY_VALUE_HEADS, head_group, HEAD_SIZE)
    index_blocks = key_index.reshape(item_count, block_span)
    seg_blocks = segs.reshape(item_count, block_span)
    scale = 1.0 / math.sqrt(HEAD_SIZE)

    def attend(item):
        query_block, query_index, query_seg = item
        scores = jnp.einsum('qhgd,khd->hgqk', query_block, key_low, precision=HIGH) * scale
        scores = low_back(scores)
        allowed = (key_index[None, :] <= query_index[:, None]) & (query_seg[:, None] == segs[None, :])
        scores = jnp.where(allowed[None, None], scores, NEG)
        probs = jax.nn.softmax(scores, axis=-1)
        return jnp.einsum('hgqk,khd->qhgd', low(probs), value_reduced, precision=HIGH)
    context = lax.map(jax.checkpoint(attend), (query_block_list, index_blocks, seg_blocks))
    context_low = low_back(low(context.reshape(span_length, QUERY_HEAD_COUNT * HEAD_SIZE)))
    middle = resid + low_back(matrix_product(context_low, w_out))
    normed_ffn = low(rms_norm(middle, ffn_gain))
    gate = low_back(matrix_product(normed_ffn, w_gate))
    upper = low_back(matrix_product(normed_ffn, w_up))
    hidden = low(jax.nn.silu(gate) * upper)
    return middle + low_back(matrix_product(hidden, w_down))

def reference(tokens, segments, cotangent, attn_gain, w_query, key_matrix, value_matrix, w_out, query_gain, key_gain, ffn_gain, w_gate, w_up, w_down):
    params = (attn_gain, w_query, key_matrix, value_matrix, w_out, query_gain, key_gain, ffn_gain, w_gate, w_up, w_down)
    params = tuple((value.astype(jnp.float32) for value in params))

    def one(totals, item):
        seq_tokens, segs, seq_grad = item

        def apply(inputs, *weights):
            return layer(inputs, segs, *weights)
        result, pullback = jax.vjp(apply, seq_tokens.astype(jnp.float32), *params)
        grads = pullback(seq_grad.astype(jnp.float32))
        totals = tuple((left + right for left, right in zip(totals, grads[1:])))
        return (totals, (result.astype(jnp.bfloat16), grads[0]))
    zeros = tuple((jnp.zeros_like(value) for value in params))
    totals, (outputs, input_grad) = lax.scan(one, zeros, (tokens, segments, cotangent))
    return (outputs, input_grad, totals[0], totals[1], totals[2], totals[3], totals[4], totals[5], totals[6], totals[7], totals[8], totals[9], totals[10])
```

```python
import functools
import math

import jax
import jax.numpy as jnp
from jax import lax
from jax.experimental import pallas as pl
from jax.experimental.pallas import tpu as pltpu
from jax.sharding import PartitionSpec as P

EPS = 1e-06
ROPE_BASE = 1000000.0
NEG = -1e30
DOC_MAX = 512
QB = 128

f32 = jnp.float32
bf16 = jnp.bfloat16


def mm(a, b, ca, cb):
    return lax.dot_general(a, b, (((ca,), (cb,)), ((), ())), preferred_element_type=f32)


def head_norm(x, gain):
    scale = lax.rsqrt(jnp.mean(x * x, axis=-1, keepdims=True) + EPS)
    return x * scale * gain, scale


def rotate(u, cosine, sine):
    return u * cosine + pltpu.roll(u, u.shape[-1] // 2, axis=1) * sine


def rotate_back(r, cosine, sine):
    return r * cosine - pltpu.roll(r, r.shape[-1] // 2, axis=1) * sine


def mask_bias(segc, segr, lo, halo, width):
    row = lax.broadcasted_iota(jnp.int32, (QB, width), 0)
    col = lax.broadcasted_iota(jnp.int32, (QB, width), 1)
    same = segc[lo : lo + QB, :] == segr[:, lo : lo + width]
    return jnp.where(same & (col <= row + halo), 0.0, NEG)


def attend_kernel(group, halo, q_ref, kv_ref, cos_ref, sin_ref, segc_ref, segr_ref, qg_ref, kg_ref, ctx_ref):
    hd = cos_ref.shape[1]
    rows = q_ref.shape[0]
    width = halo + QB
    scale = 1.0 / math.sqrt(hd)
    cosine, sine = cos_ref[...], sin_ref[...]
    kn, _ = head_norm(kv_ref[:, :hd], kg_ref[...])
    k_low = rotate(kn, cosine, sine).astype(bf16)
    v_low = kv_ref[:, hd:].astype(bf16)
    for i in range(rows // QB):
        lo = i * QB
        bias = mask_bias(segc_ref[0], segr_ref[0], lo, halo, width)
        qs = []
        for h in range(group):
            qn, _ = head_norm(q_ref[lo : lo + QB, h * hd : (h + 1) * hd], qg_ref[...])
            at = halo + lo
            qs.append(rotate(qn, cosine[at : at + QB], sine[at : at + QB]).astype(bf16))
        q_low = jnp.concatenate(qs, axis=0)
        s = mm(q_low, k_low[lo : lo + width], 1, 1)
        e = jnp.exp(s * scale + jnp.concatenate([bias] * group, axis=0))
        p = (e * (1.0 / jnp.sum(e, axis=-1, keepdims=True))).astype(bf16)
        c = mm(p, v_low[lo : lo + width], 1, 0).astype(bf16)
        for h in range(group):
            ctx_ref[lo : lo + QB, h * hd : (h + 1) * hd] = c[h * QB : (h + 1) * QB]


def attend_back_kernel(
    group, halo, q_ref, kv_ref, dc_ref, cos_ref, sin_ref, segc_ref, segr_ref, qg_ref, kg_ref,
    dq_ref, dkv_ref, qgg_ref, kgg_ref, dk_ref, dv_ref,
):
    hd = cos_ref.shape[1]
    rows = q_ref.shape[0]
    width = halo + QB
    scale = 1.0 / math.sqrt(hd)
    cosine, sine = cos_ref[...], sin_ref[...]
    q_gain, k_gain = qg_ref[...], kg_ref[...]

    @pl.when((pl.program_id(0) == 0) & (pl.program_id(1) == 0))
    def _():
        qgg_ref[...] = jnp.zeros_like(qgg_ref)
        kgg_ref[...] = jnp.zeros_like(kgg_ref)

    k_raw = kv_ref[:, :hd]
    kn, k_scale = head_norm(k_raw, k_gain)
    k_low = rotate(kn, cosine, sine).astype(bf16)
    v_low = kv_ref[:, hd:].astype(bf16)
    dk_ref[...] = jnp.zeros_like(dk_ref)
    dv_ref[...] = jnp.zeros_like(dv_ref)
    q_gain_grad = jnp.zeros((1, hd), f32)
    for i in range(rows // QB):
        lo = i * QB
        at = halo + lo
        cq, sq = cosine[at : at + QB], sine[at : at + QB]
        bias = mask_bias(segc_ref[0], segr_ref[0], lo, halo, width)
        raws, scales, lows, dcs = [], [], [], []
        for h in range(group):
            raw = q_ref[lo : lo + QB, h * hd : (h + 1) * hd]
            qn, q_scale = head_norm(raw, q_gain)
            raws.append(raw)
            scales.append(q_scale)
            lows.append(rotate(qn, cq, sq).astype(bf16))
            dcs.append(dc_ref[lo : lo + QB, h * hd : (h + 1) * hd])
        q_low = jnp.concatenate(lows, axis=0)
        dc = jnp.concatenate(dcs, axis=0)
        kw, vw = k_low[lo : lo + width], v_low[lo : lo + width]
        s = mm(q_low, kw, 1, 1)
        e = jnp.exp(s * scale + jnp.concatenate([bias] * group, axis=0))
        p = e * (1.0 / jnp.sum(e, axis=-1, keepdims=True))
        dp = mm(dc, vw, 1, 1)
        inner = jnp.sum(p * dp, axis=-1, keepdims=True)
        ds = (p * (dp - inner)).astype(bf16)
        dq = mm(ds, kw, 1, 0) * scale
        dk_ref[lo : lo + width, :] += mm(ds, q_low, 0, 0)
        dv_ref[lo : lo + width, :] += mm(p.astype(bf16), dc, 0, 0)
        for h in range(group):
            rot = rotate_back(dq[h * QB : (h + 1) * QB], cq, sq)
            raw, sc = raws[h], scales[h]
            b = rot * q_gain
            q_gain_grad += jnp.sum(rot * raw * sc, axis=0, keepdims=True)
            grad = sc * b - raw * (sc * sc * sc * jnp.mean(b * raw, axis=-1, keepdims=True))
            dq_ref[lo : lo + QB, h * hd : (h + 1) * hd] = grad.astype(bf16)
    qgg_ref[...] += q_gain_grad
    rot = rotate_back(dk_ref[...] * scale, cosine, sine)
    b = rot * k_gain
    kgg_ref[...] += jnp.sum(rot * k_raw * k_scale, axis=0, keepdims=True)
    grad = k_scale * b - k_raw * (k_scale * k_scale * k_scale * jnp.mean(b * k_raw, axis=-1, keepdims=True))
    dkv_ref[:, :hd] = grad.astype(bf16)
    dkv_ref[:, hd:] = dv_ref[...].astype(bf16)


def attention_specs(seqs, rows, keys, group, hd):
    return [
        pl.BlockSpec((rows, group * hd), lambda j, g: (j, g)),
        pl.BlockSpec((keys, 2 * hd), lambda j, g: (j, g)),
    ], [
        pl.BlockSpec((keys, hd), lambda j, g: (0, 0)),
        pl.BlockSpec((keys, hd), lambda j, g: (0, 0)),
        pl.BlockSpec((1, rows, 1), lambda j, g: (j, 0, 0)),
        pl.BlockSpec((1, 1, keys), lambda j, g: (j, 0, 0)),
        pl.BlockSpec((1, hd), lambda j, g: (0, 0)),
        pl.BlockSpec((1, hd), lambda j, g: (0, 0)),
    ]


def attend(q_raw, kv_raw, tables, seqs, rows, keys, group, hd):
    heads = kv_raw.shape[1] // (2 * hd)
    first, rest = attention_specs(seqs, rows, keys, group, hd)
    pairs = seqs * heads * group * rows * (keys - rows + QB)
    return pl.pallas_call(
        functools.partial(attend_kernel, group, keys - rows),
        grid=(seqs, heads),
        in_specs=first + rest,
        out_specs=pl.BlockSpec((rows, group * hd), lambda j, g: (j, g)),
        out_shape=jax.ShapeDtypeStruct(q_raw.shape, bf16),
        cost_estimate=pl.CostEstimate(
            flops=4 * pairs * hd, bytes_accessed=q_raw.size * 6 + kv_raw.size * 4, transcendentals=pairs
        ),
        name="attend",
    )(q_raw, kv_raw, *tables)


def attend_back(q_raw, kv_raw, context_grad, tables, seqs, rows, keys, group, hd):
    heads = kv_raw.shape[1] // (2 * hd)
    first, rest = attention_specs(seqs, rows, keys, group, hd)
    pairs = seqs * heads * group * rows * (keys - rows + QB)
    gain_spec = pl.BlockSpec((1, hd), lambda j, g: (0, 0))
    return pl.pallas_call(
        functools.partial(attend_back_kernel, group, keys - rows),
        grid=(seqs, heads),
        in_specs=first + [first[0]] + rest,
        out_specs=[first[0], first[1], gain_spec, gain_spec],
        out_shape=[
            jax.ShapeDtypeStruct(q_raw.shape, bf16),
            jax.ShapeDtypeStruct(kv_raw.shape, bf16),
            jax.ShapeDtypeStruct((1, hd), f32),
            jax.ShapeDtypeStruct((1, hd), f32),
        ],
        scratch_shapes=[pltpu.VMEM((keys, hd), f32), pltpu.VMEM((keys, hd), f32)],
        cost_estimate=pl.CostEstimate(
            flops=10 * pairs * hd, bytes_accessed=q_raw.size * 8 + kv_raw.size * 6, transcendentals=pairs
        ),
        name="attend_back",
    )(q_raw, kv_raw, context_grad, *tables)


def feed_kernel(x_ref, u_ref, wgu_ref, wd_ref, hid_ref, gug_ref, ng_ref, out_ref):
    n = wd_ref.shape[0]
    wgu, wd, u = wgu_ref[...], wd_ref[...], u_ref[...]
    gu = mm(x_ref[...], wgu, 1, 0)
    hg = mm(u, wd, 1, 1)
    gate, upper = gu[:, :n], gu[:, n:]
    sig = 1.0 / (1.0 + jnp.exp(-gate))
    act = gate * sig
    hidden = (act * upper).astype(bf16)
    hid_ref[...] = hidden
    gg = (hg * upper * sig * (1.0 + gate * (1.0 - sig))).astype(bf16)
    ug = (hg * act).astype(bf16)
    gug_ref[:, :n] = gg
    gug_ref[:, n:] = ug
    ng_ref[...] = (mm(gg, wgu[:, :n], 1, 1) + mm(ug, wgu[:, n:], 1, 1)).astype(bf16)
    out_ref[...] = mm(hidden, wd, 1, 0).astype(bf16)


def feed(x, u, wgu, wd, block):
    t, d = x.shape
    n = wd.shape[0]
    row = lambda cols: pl.BlockSpec((block, cols), lambda i: (i, 0))
    whole = lambda a: pl.BlockSpec(a.shape, lambda i: (0, 0), pipeline_mode=pl.Buffered(1))
    return pl.pallas_call(
        feed_kernel,
        grid=(t // block,),
        in_specs=[row(d), row(d), whole(wgu), whole(wd)],
        out_specs=[row(n), row(2 * n), row(d), row(d)],
        out_shape=[
            jax.ShapeDtypeStruct((t, n), bf16),
            jax.ShapeDtypeStruct((t, 2 * n), bf16),
            jax.ShapeDtypeStruct((t, d), bf16),
            jax.ShapeDtypeStruct((t, d), bf16),
        ],
        cost_estimate=pl.CostEstimate(
            flops=14 * t * d * n, bytes_accessed=2 * (4 * t * d + 3 * t * n + 3 * d * n), transcendentals=t * n
        ),
        name="feed",
    )(x, u, wgu, wd)


def row_norm(values, gain):
    scale = lax.rsqrt(jnp.mean(values * values, axis=-1, keepdims=True) + EPS)
    return (values * scale * gain).astype(bf16), scale


def row_norm_back(values, scale, gain, upstream):
    weighted = upstream * gain
    inner = jnp.mean(weighted * values, axis=-1, keepdims=True)
    return scale * weighted - values * (scale * scale * scale * inner)


def build(mesh):
    F, Z = mesh.shape["fsdp"], mesh.shape["ctx"]
    C = F // 2
    assert F == 2 * C and F & (F - 1) == 0 and Z & (Z - 1) == 0 and Z > 1
    chip_bits = [2 << i for i in range(C.bit_length() - 1)]
    z_bits = [1 << i for i in range(Z.bit_length() - 1)]
    sizes = {"fsdp": F, "ctx": Z}

    def hop(x, axis, bit):
        return lax.ppermute(x, axis, [(i, i ^ bit) for i in range(sizes[axis])])

    def shift(x, by):
        return lax.ppermute(x, "ctx", [(i, i + by) for i in range(Z) if 0 <= i + by < Z])

    def gather_chips(piece, c):
        r, n = piece.shape
        out = jnp.zeros((C * r, n), piece.dtype)
        place = lambda buf, part, rel, off=0: lax.dynamic_update_slice(buf, part, ((c ^ rel) * r + off, 0))
        if C == 4:
            x, y = hop(piece, "fsdp", 2), hop(piece, "fsdp", 4)
            h = r // 2
            da, db = hop(x[:h], "fsdp", 4), hop(y[h:], "fsdp", 2)
            for part, rel, off in ((piece, 0, 0), (x, 1, 0), (y, 2, 0), (da, 3, 0), (db, 3, h)):
                out = place(out, part, rel, off)
            return out
        parts = [piece]
        for bit in chip_bits:
            parts = parts + [hop(p, "fsdp", bit) for p in parts]
        for rel, part in enumerate(parts):
            out = place(out, part, rel)
        return out

    def scatter_chips(full, c):
        r = full.shape[0] // C
        parts = [lax.dynamic_slice_in_dim(full, (c ^ rel) * r, r) for rel in range(C)]
        if C == 4:
            h = r // 2
            ra, rb = hop(parts[3][:h], "fsdp", 4), hop(parts[3][h:], "fsdp", 2)
            add = lambda a, b: (a.astype(f32) + b.astype(f32)).astype(bf16)
            px = jnp.concatenate([add(parts[1][:h], ra), parts[1][h:]], axis=0)
            py = jnp.concatenate([parts[2][:h], add(parts[2][h:], rb)], axis=0)
            rx, ry = hop(px, "fsdp", 2), hop(py, "fsdp", 4)
            return parts[0].astype(f32) + rx.astype(f32) + ry.astype(f32)
        parts = [p.astype(f32) for p in parts]
        for bit in reversed(chip_bits):
            half = len(parts) // 2
            got = [hop(p.astype(bf16), "fsdp", bit) for p in parts[half:]]
            parts = [p + g.astype(f32) for p, g in zip(parts[:half], got)]
        return parts[0]

    def z_sum(b, bits):
        for bit in bits:
            b = (b.astype(f32) + hop(b, "ctx", bit).astype(f32)).astype(bf16)
        return b

    def z_sum_split(own, zb):
        h = own.shape[0] // 2
        top, bottom = own[:h], own[h:]
        mine, theirs = jnp.where(zb == 0, top, bottom), jnp.where(zb == 0, bottom, top)
        mine = mine.astype(f32) + hop(theirs.astype(bf16), "ctx", 1).astype(f32)
        b = z_sum(mine.astype(bf16), z_bits[1:])
        o = hop(b, "ctx", 1)
        return jnp.where(zb == 0, jnp.concatenate([b, o]), jnp.concatenate([o, b]))

    def body(
        tokens, segments, cotangent, attn_gain, w_query, key_matrix, value_matrix, w_out,
        query_gain, key_gain, ffn_gain, w_gate, w_up, w_down,
    ):
        me = lax.axis_index("fsdp")
        core, c = me % 2, me // 2
        zb = lax.axis_index("ctx") % 2
        R, D = tokens.shape[1:]
        hd = query_gain.shape[0]
        heads, kv_heads = w_query.shape[1] // hd, key_matrix.shape[1] // hd
        group = heads // F
        kv_split = kv_heads == F
        assert heads % F == 0 and (kv_split or (kv_heads == C and heads == F))
        halos = -(-(DOC_MAX - 1) // R)
        K = (halos + 1) * R
        qc = group * hd
        dr = w_query.shape[0]
        FB = w_down.shape[0]
        FS = FB // 2
        swap = lambda x: hop(x, "fsdp", 1)
        by_core = lambda a, b: jnp.where(core == 0, a, b)

        gains = jnp.stack([attn_gain, ffn_gain])[None]
        other = swap(gains)
        gains = by_core(jnp.concatenate([gains, other]), jnp.concatenate([other, gains]))
        for bit in chip_bits:
            other = hop(gains, "fsdp", bit)
            gains = jnp.where(
                me & bit == 0, jnp.concatenate([gains, other]), jnp.concatenate([other, gains])
            )
        gain_attn = gains[:, 0].reshape(1, D).astype(f32)
        gain_ffn = gains[:, 1].reshape(1, D).astype(f32)

        def columns(w, blocks):
            return jnp.concatenate([w[:, s : s + n] for s, n in blocks], axis=1)

        def qkv_of(k):
            q = columns(w_query, [((2 * i + k) * qc, qc) for i in range(C)])
            kv = []
            for i in range(C):
                b = (2 * i + k if kv_split else i) * hd
                kv += [key_matrix[:, b : b + hd], value_matrix[:, b : b + hd]]
            return jnp.concatenate([q] + kv, axis=1)

        def gu_of(k):
            pick = lambda w, z: columns(w, [((2 * i + k) * FB + z * FS, FS) for i in range(C)])
            return jnp.concatenate(
                [jnp.where(zb == 0, pick(w, 0), pick(w, 1)) for w in (w_gate, w_up)], axis=1
            )

        def chip_rows(of):
            even, odd = of(0), of(1)
            mine, got = by_core(even, odd), swap(by_core(odd, even))
            return by_core(jnp.concatenate([mine, got]), jnp.concatenate([got, mine]))

        w_qkv = gather_chips(chip_rows(qkv_of), c)
        wq, wkv = w_qkv[:, : C * qc], w_qkv[:, C * qc :]

        pad = 16
        seg_rows = jnp.zeros((pad, D), bf16).at[0, :R].set((segments[0] + 1).astype(bf16))
        cur = jnp.concatenate([tokens[0], seg_rows])
        window = [cur]
        for _ in range(halos):
            cur = shift(cur, 1)
            window.insert(0, cur)
        window = jnp.stack(window)
        window = jnp.stack([window, swap(window)])
        seg = window[:, :, R, :R].reshape(2, K).astype(jnp.int32)
        resid = window[:, :, :R].reshape(2, K, D).astype(f32)

        upstream = cotangent[0].astype(f32)
        u = jnp.stack([cotangent[0], hop(cotangent[0], "ctx", 1)])
        u4 = jnp.concatenate([u, swap(u)]).reshape(4 * R, D)

        half = hd // 2
        freq = 1.0 / ROPE_BASE ** (jnp.arange(half, dtype=f32) * 2.0 / hd)
        angle = jnp.arange(K, dtype=f32)[:, None] * freq[None, :]
        cosine, sine = jnp.cos(angle), jnp.sin(angle)
        tables = (
            jnp.concatenate([cosine, cosine], axis=1),
            jnp.concatenate([-sine, sine], axis=1),
            seg[:, K - R :, None],
            seg[:, None, :],
            query_gain.astype(f32)[None],
            key_gain.astype(f32)[None],
        )

        normed, scale_attn = row_norm(resid, gain_attn)
        normed_own = normed[:, K - R :].reshape(2 * R, D)
        normed_all = normed.reshape(2 * K, D)
        q_raw = mm(normed_own, wq, 1, 0)
        kv_raw = mm(normed_all, wkv, 1, 0)
        context = attend(q_raw, kv_raw, tables, 2, R, K, group, hd)
        w_o = gather_chips(w_out, c)
        part = mm(context, w_o, 1, 0)
        middle = resid[0, K - R :] + part[:R] + swap(part[R:].astype(bf16)).astype(f32)

        w_gu = gather_chips(chip_rows(gu_of), c)
        w_d = gather_chips(jnp.where(zb == 0, w_down[:FS], w_down[FS:]), c)
        nf, scale_ffn = row_norm(middle, gain_ffn)
        x = jnp.stack([nf, hop(nf, "ctx", 1)])
        x4 = jnp.concatenate([x, swap(x)]).reshape(4 * R, D)
        hidden, gug, ng, out = feed(x4, u4, w_gu, w_d, R)

        def token_sum(parts):
            parts = parts.reshape(4, R, D)
            s = parts[:2].astype(f32) + swap(parts[2:]).astype(f32)
            return s[0] + hop(s[1].astype(bf16), "ctx", 1).astype(f32)

        normed_grad = token_sum(ng)
        output = (middle + token_sum(out)).astype(bf16)
        ffn_gain_term = jnp.sum(normed_grad * middle * scale_ffn, axis=0)
        middle_grad = upstream + row_norm_back(middle, scale_ffn, gain_ffn, normed_grad)

        d_down = scatter_chips(mm(hidden, u4, 0, 0).astype(bf16), c)
        d_down = z_sum(d_down.astype(bf16), z_bits[1:])
        o = hop(d_down, "ctx", 1)
        d_down = jnp.where(zb == 0, jnp.concatenate([d_down, o]), jnp.concatenate([o, d_down])).astype(f32)

        def core_rows(rows):
            top, bottom = rows[:dr], rows[dr:]
            mine, theirs = by_core(top, bottom), by_core(bottom, top)
            return mine, swap(theirs.astype(bf16)).astype(f32)

        def by_parity(mine, other):
            return by_core(mine, other), by_core(other, mine)

        mine, got = core_rows(scatter_chips(mm(x4, gug, 0, 0).astype(bf16), c))
        mine = z_sum(jnp.concatenate([mine, got]).astype(bf16), z_bits[1:])
        o = hop(mine, "ctx", 1)
        z0, z1 = jnp.where(zb == 0, mine, o), jnp.where(zb == 0, o, mine)
        quarters = [by_parity(q[:dr], q[dr:]) for q in (z0, z1)]

        def unit_columns(base):
            cols = []
            for i in range(C):
                for k in range(2):
                    for z in range(2):
                        s = base + i * FS
                        cols.append(quarters[z][k][:, s : s + FS])
            return jnp.concatenate(cols, axis=1).astype(f32)

        d_gate, d_up = unit_columns(0), unit_columns(C * FS)

        ml = middle_grad.astype(bf16)
        ml2 = jnp.concatenate([ml, swap(ml)])
        context_grad = mm(ml2, w_o, 1, 1).astype(bf16)
        d_out = z_sum_split(scatter_chips(mm(context, ml2, 0, 0).astype(bf16), c), zb).astype(f32)
        dq, dkv, q_gain_term, k_gain_term = attend_back(
            q_raw, kv_raw, context_grad, tables, 2, R, K, group, hd
        )
        d_qkv = jnp.concatenate(
            [mm(normed_own, dq, 0, 0).astype(bf16), mm(normed_all, dkv, 0, 0).astype(bf16)], axis=1
        )
        own_rows = mm(dq, wq, 1, 1).reshape(2, R, D)
        attn_grad = mm(dkv, wkv, 1, 1).reshape(2, K, D)
        attn_grad = attn_grad + jnp.pad(own_rows, ((0, 0), (K - R, 0), (0, 0)))
        attn_grad = attn_grad[0] + swap(attn_grad[1].astype(bf16)).astype(f32)
        attn_gain_term = jnp.sum(attn_grad * resid[0] * scale_attn[0], axis=0)
        carry = attn_grad[:R]
        for i in range(1, halos + 1):
            carry = attn_grad[i * R : (i + 1) * R] + shift(carry.astype(bf16), -1).astype(f32)
        input_grad = middle_grad + row_norm_back(
            resid[0, K - R :], scale_attn[0, K - R :], gain_attn, carry
        )

        mine, got = core_rows(scatter_chips(d_qkv, c))
        if kv_split:
            full = z_sum_split(jnp.concatenate([mine, got]), zb).astype(f32)
            even, odd = by_parity(full[:dr], full[dr:])
        else:
            kv = mine[:, C * qc :] + got[:, C * qc :]
            full = z_sum_split(jnp.concatenate([mine[:, : C * qc], got[:, : C * qc], kv], axis=1), zb).astype(f32)
            even, odd = by_parity(full[:, : C * qc], full[:, C * qc : 2 * C * qc])
            kv = full[:, 2 * C * qc :]
        d_query = jnp.concatenate(
            [p[:, i * qc : (i + 1) * qc] for i in range(C) for p in (even, odd)], axis=1
        )
        if kv_split:
            pick = lambda off: jnp.concatenate(
                [
                    p[:, C * qc + 2 * i * hd + off : C * qc + 2 * i * hd + off + hd]
                    for i in range(C)
                    for p in (even, odd)
                ],
                axis=1,
            )
        else:
            pick = lambda off: jnp.concatenate(
                [kv[:, 2 * i * hd + off : 2 * i * hd + off + hd] for i in range(C)], axis=1
            )
        d_key, d_value = pick(0), pick(hd)

        small = jnp.concatenate([q_gain_term[0], k_gain_term[0], ffn_gain_term, attn_gain_term])
        small = small.reshape(-1, 128)
        for axis, bits in (("fsdp", [1] + chip_bits), ("ctx", z_bits)):
            for bit in bits:
                small = small + hop(small, axis, bit)
        small = small.reshape(-1)
        own_gain = lambda base: lax.dynamic_slice_in_dim(small, base + me * dr, dr)
        return (
            output[None],
            input_grad[None],
            own_gain(2 * hd + D),
            d_query,
            d_key,
            d_value,
            d_out,
            small[:hd],
            small[hd : 2 * hd],
            own_gain(2 * hd),
            d_gate,
            d_up,
            d_down,
        )

    return body


def solution(mesh):
    row = P("fsdp", None)
    token = P("fsdp", "ctx", None)
    in_specs = (token, P("fsdp", "ctx"), token, P("fsdp"), row, row, row, row, P(), P(), P("fsdp"), row, row, row)
    out_specs = (token, token, P("fsdp"), row, row, row, row, P(), P(), P("fsdp"), row, row, row)
    return jax.shard_map(build(mesh), mesh=mesh, in_specs=in_specs, out_specs=out_specs, check_vma=False)
```

```python
import functools
import math

import jax
import jax.numpy as jnp
from jax import lax
from jax.experimental import pallas as pl
from jax.experimental.pallas import tpu as pltpu
from jax.sharding import PartitionSpec as P

EPS = 1e-06
ROPE_BASE = 1000000.0
NEG = -1e30
DOC_MAX = 512
QB = 128

f32 = jnp.float32
bf16 = jnp.bfloat16


def mm(a, b, ca, cb):
    return lax.dot_general(a, b, (((ca,), (cb,)), ((), ())), preferred_element_type=f32)


def head_norm(x, gain):
    scale = lax.rsqrt(jnp.mean(x * x, axis=-1, keepdims=True) + EPS)
    return x * scale * gain, scale


def rotate(u, cosine, sine):
    return u * cosine + pltpu.roll(u, u.shape[-1] // 2, axis=1) * sine


def rotate_back(r, cosine, sine):
    return r * cosine - pltpu.roll(r, r.shape[-1] // 2, axis=1) * sine


def mask_bias(segc, segr, lo, halo, width):
    row = lax.broadcasted_iota(jnp.int32, (QB, width), 0)
    col = lax.broadcasted_iota(jnp.int32, (QB, width), 1)
    same = segc[lo : lo + QB, :] == segr[:, lo : lo + width]
    return jnp.where(same & (col <= row + halo), 0.0, NEG)


def attend_kernel(group, halo, q_ref, kv_ref, cos_ref, sin_ref, segc_ref, segr_ref, qg_ref, kg_ref, ctx_ref):
    hd = cos_ref.shape[1]
    rows = q_ref.shape[0]
    width = halo + QB
    scale = 1.0 / math.sqrt(hd)
    cosine, sine = cos_ref[...], sin_ref[...]
    kn, _ = head_norm(kv_ref[:, :hd], kg_ref[...])
    k_low = rotate(kn, cosine, sine).astype(bf16)
    v_low = kv_ref[:, hd:].astype(bf16)
    for i in range(rows // QB):
        lo = i * QB
        bias = mask_bias(segc_ref[0], segr_ref[0], lo, halo, width)
        qs = []
        for h in range(group):
            qn, _ = head_norm(q_ref[lo : lo + QB, h * hd : (h + 1) * hd], qg_ref[...])
            at = halo + lo
            qs.append(rotate(qn, cosine[at : at + QB], sine[at : at + QB]).astype(bf16))
        q_low = jnp.concatenate(qs, axis=0)
        s = mm(q_low, k_low[lo : lo + width], 1, 1)
        e = jnp.exp(s * scale + jnp.concatenate([bias] * group, axis=0))
        p = (e * (1.0 / jnp.sum(e, axis=-1, keepdims=True))).astype(bf16)
        c = mm(p, v_low[lo : lo + width], 1, 0).astype(bf16)
        for h in range(group):
            ctx_ref[lo : lo + QB, h * hd : (h + 1) * hd] = c[h * QB : (h + 1) * QB]


def attend_back_kernel(
    group, halo, q_ref, kv_ref, dc_ref, cos_ref, sin_ref, segc_ref, segr_ref, qg_ref, kg_ref,
    dq_ref, dkv_ref, qgg_ref, kgg_ref, dk_ref, dv_ref,
):
    hd = cos_ref.shape[1]
    rows = q_ref.shape[0]
    width = halo + QB
    scale = 1.0 / math.sqrt(hd)
    cosine, sine = cos_ref[...], sin_ref[...]
    q_gain, k_gain = qg_ref[...], kg_ref[...]

    @pl.when((pl.program_id(0) == 0) & (pl.program_id(1) == 0))
    def _():
        qgg_ref[...] = jnp.zeros_like(qgg_ref)
        kgg_ref[...] = jnp.zeros_like(kgg_ref)

    k_raw = kv_ref[:, :hd]
    kn, k_scale = head_norm(k_raw, k_gain)
    k_low = rotate(kn, cosine, sine).astype(bf16)
    v_low = kv_ref[:, hd:].astype(bf16)
    dk_ref[...] = jnp.zeros_like(dk_ref)
    dv_ref[...] = jnp.zeros_like(dv_ref)
    q_gain_grad = jnp.zeros((1, hd), f32)
    for i in range(rows // QB):
        lo = i * QB
        at = halo + lo
        cq, sq = cosine[at : at + QB], sine[at : at + QB]
        bias = mask_bias(segc_ref[0], segr_ref[0], lo, halo, width)
        raws, scales, lows, dcs = [], [], [], []
        for h in range(group):
            raw = q_ref[lo : lo + QB, h * hd : (h + 1) * hd]
            qn, q_scale = head_norm(raw, q_gain)
            raws.append(raw)
            scales.append(q_scale)
            lows.append(rotate(qn, cq, sq).astype(bf16))
            dcs.append(dc_ref[lo : lo + QB, h * hd : (h + 1) * hd])
        q_low = jnp.concatenate(lows, axis=0)
        dc = jnp.concatenate(dcs, axis=0)
        kw, vw = k_low[lo : lo + width], v_low[lo : lo + width]
        s = mm(q_low, kw, 1, 1)
        e = jnp.exp(s * scale + jnp.concatenate([bias] * group, axis=0))
        p = e * (1.0 / jnp.sum(e, axis=-1, keepdims=True))
        dp = mm(dc, vw, 1, 1)
        inner = jnp.sum(p * dp, axis=-1, keepdims=True)
        ds = (p * (dp - inner)).astype(bf16)
        dq = mm(ds, kw, 1, 0) * scale
        dk_ref[lo : lo + width, :] += mm(ds, q_low, 0, 0)
        dv_ref[lo : lo + width, :] += mm(p.astype(bf16), dc, 0, 0)
        for h in range(group):
            rot = rotate_back(dq[h * QB : (h + 1) * QB], cq, sq)
            raw, sc = raws[h], scales[h]
            b = rot * q_gain
            q_gain_grad += jnp.sum(rot * raw * sc, axis=0, keepdims=True)
            grad = sc * b - raw * (sc * sc * sc * jnp.mean(b * raw, axis=-1, keepdims=True))
            dq_ref[lo : lo + QB, h * hd : (h + 1) * hd] = grad.astype(bf16)
    qgg_ref[...] += q_gain_grad
    rot = rotate_back(dk_ref[...] * scale, cosine, sine)
    b = rot * k_gain
    kgg_ref[...] += jnp.sum(rot * k_raw * k_scale, axis=0, keepdims=True)
    grad = k_scale * b - k_raw * (k_scale * k_scale * k_scale * jnp.mean(b * k_raw, axis=-1, keepdims=True))
    dkv_ref[:, :hd] = grad.astype(bf16)
    dkv_ref[:, hd:] = dv_ref[...].astype(bf16)


def attention_specs(seqs, rows, keys, group, hd):
    return [
        pl.BlockSpec((rows, group * hd), lambda j, g: (j, g)),
        pl.BlockSpec((keys, 2 * hd), lambda j, g: (j, g)),
    ], [
        pl.BlockSpec((keys, hd), lambda j, g: (0, 0)),
        pl.BlockSpec((keys, hd), lambda j, g: (0, 0)),
        pl.BlockSpec((1, rows, 1), lambda j, g: (j, 0, 0)),
        pl.BlockSpec((1, 1, keys), lambda j, g: (j, 0, 0)),
        pl.BlockSpec((1, hd), lambda j, g: (0, 0)),
        pl.BlockSpec((1, hd), lambda j, g: (0, 0)),
    ]


def attend(q_raw, kv_raw, tables, seqs, rows, keys, group, hd):
    heads = kv_raw.shape[1] // (2 * hd)
    first, rest = attention_specs(seqs, rows, keys, group, hd)
    pairs = seqs * heads * group * rows * (keys - rows + QB)
    return pl.pallas_call(
        functools.partial(attend_kernel, group, keys - rows),
        grid=(seqs, heads),
        in_specs=first + rest,
        out_specs=pl.BlockSpec((rows, group * hd), lambda j, g: (j, g)),
        out_shape=jax.ShapeDtypeStruct(q_raw.shape, bf16),
        cost_estimate=pl.CostEstimate(
            flops=4 * pairs * hd, bytes_accessed=q_raw.size * 6 + kv_raw.size * 4, transcendentals=pairs
        ),
        compiler_params=pltpu.CompilerParams(vmem_limit_bytes=20 << 20),
        name="attend",
    )(q_raw, kv_raw, *tables)


def attend_back(q_raw, kv_raw, context_grad, tables, seqs, rows, keys, group, hd):
    heads = kv_raw.shape[1] // (2 * hd)
    first, rest = attention_specs(seqs, rows, keys, group, hd)
    pairs = seqs * heads * group * rows * (keys - rows + QB)
    gain_spec = pl.BlockSpec((1, hd), lambda j, g: (0, 0))
    return pl.pallas_call(
        functools.partial(attend_back_kernel, group, keys - rows),
        grid=(seqs, heads),
        in_specs=first + [first[0]] + rest,
        out_specs=[first[0], first[1], gain_spec, gain_spec],
        out_shape=[
            jax.ShapeDtypeStruct(q_raw.shape, bf16),
            jax.ShapeDtypeStruct(kv_raw.shape, bf16),
            jax.ShapeDtypeStruct((1, hd), f32),
            jax.ShapeDtypeStruct((1, hd), f32),
        ],
        scratch_shapes=[pltpu.VMEM((keys, hd), f32), pltpu.VMEM((keys, hd), f32)],
        cost_estimate=pl.CostEstimate(
            flops=10 * pairs * hd,
            bytes_accessed=seqs * heads * (8 * rows * group * hd + 12 * keys * hd),
            transcendentals=pairs,
        ),
        compiler_params=pltpu.CompilerParams(vmem_limit_bytes=28 << 20),
        name="attend_back",
    )(q_raw, kv_raw, context_grad, *tables)


def diagonal(gain_ref):
    n = gain_ref.shape[1]
    row = lax.broadcasted_iota(jnp.int32, (n, n), 0)
    col = lax.broadcasted_iota(jnp.int32, (n, n), 1)
    return jnp.where(row == col, gain_ref[...].astype(f32), 0.0).astype(bf16)


def select_kernel(chips, qc, hd, split, core_ref, gain_ref, wq_ref, wk_ref, wv_ref, mine_ref, theirs_ref):
    gain = diagonal(gain_ref)
    for out_ref, k in ((mine_ref, core_ref[0]), (theirs_ref, 1 - core_ref[0])):
        for i in range(chips):
            at = pl.ds(pl.multiple_of((2 * i + k) * qc, qc), qc)
            out_ref[:, i * qc : (i + 1) * qc] = mm(gain, wq_ref[:, at], 1, 0).astype(bf16)
            at = pl.ds(pl.multiple_of((2 * i + k if split else i) * hd, hd), hd)
            base = chips * qc + 2 * i * hd
            out_ref[:, base : base + hd] = mm(gain, wk_ref[:, at], 1, 0).astype(bf16)
            out_ref[:, base + hd : base + 2 * hd] = mm(gain, wv_ref[:, at], 1, 0).astype(bf16)


def small_call(kernel, scalars, args, outs, name):
    spec = lambda a: pl.BlockSpec(a.shape, lambda i, *_: (0,) * len(a.shape), pipeline_mode=pl.Buffered(1))
    size = lambda a: math.prod(a.shape) * a.dtype.itemsize
    return pl.pallas_call(
        kernel,
        grid_spec=pltpu.PrefetchScalarGridSpec(
            num_scalar_prefetch=1,
            grid=(1,),
            in_specs=[spec(a) for a in args],
            out_specs=[spec(o) for o in outs],
        ),
        out_shape=outs,
        cost_estimate=pl.CostEstimate(
            flops=0, bytes_accessed=sum(size(a) for a in (*args, *outs)), transcendentals=0
        ),
        compiler_params=pltpu.CompilerParams(vmem_limit_bytes=16 << 20),
        name=name,
    )(scalars, *args)


def select_qkv(core, gain, wq, wk, wv, chips, qc, hd, split):
    out = jax.ShapeDtypeStruct((wq.shape[0], chips * (qc + 2 * hd)), bf16)
    kernel = functools.partial(select_kernel, chips, qc, hd, split)
    return small_call(kernel, core[None], (gain, wq, wk, wv), (out, out), "select_qkv")


def select_units_kernel(chips, where_ref, gain_ref, wg_ref, wu_ref, mine_ref, theirs_ref):
    n = wg_ref.shape[1] // (4 * chips)
    gain = diagonal(gain_ref)
    for k in range(2):
        for z in range(2):

            @pl.when((where_ref[0] == k) & (where_ref[1] == z))
            def _():
                for out_ref, kk in ((mine_ref, k), (theirs_ref, 1 - k)):
                    for m, w_ref in enumerate((wg_ref, wu_ref)):
                        cols = [w_ref[:, (4 * i + 2 * kk + z) * n : (4 * i + 2 * kk + z + 1) * n] for i in range(chips)]
                        out = mm(gain, jnp.concatenate(cols, axis=1), 1, 0)
                        out_ref[:, m * chips * n : (m + 1) * chips * n] = out.astype(bf16)


def select_units(where, gain, wg, wu, chips):
    out = jax.ShapeDtypeStruct((wg.shape[0], wg.shape[1] // 2), bf16)
    kernel = functools.partial(select_units_kernel, chips)
    return small_call(kernel, where, (gain, wg, wu), (out, out), "select_units")


def place_units_kernel(chips, where_ref, gain_ref, a_ref, b_ref, dg_ref, du_ref):
    dr = dg_ref.shape[0]
    n = dg_ref.shape[1] // (4 * chips)
    gain = diagonal(gain_ref)
    for k in range(2):
        for z in range(2):

            @pl.when((where_ref[0] == k) & (where_ref[1] == z))
            def _():
                for m, out_ref in enumerate((dg_ref, du_ref)):
                    for i in range(chips):
                        cols = []
                        for kk in range(2):
                            for zz in range(2):
                                ref = a_ref if zz == z else b_ref
                                top = 0 if kk == k else dr
                                at = (m * chips + i) * n
                                cols.append(ref[top : top + dr, at : at + n])
                        out_ref[:, 4 * i * n : 4 * (i + 1) * n] = mm(gain, jnp.concatenate(cols, axis=1), 1, 0)


def place_units(where, gain, a, b, chips):
    out = jax.ShapeDtypeStruct((a.shape[0] // 2, 2 * a.shape[1]), f32)
    kernel = functools.partial(place_units_kernel, chips)
    return small_call(kernel, where, (gain, a, b), (out, out), "place_units")


def feed_kernel(chip_ref, xa_ref, xb_ref, ua_ref, ub_ref, wgu_ref, parts, hid_ref, gug_ref, ng_ref, out_ref, wd_ref):
    n = wd_ref.shape[0]
    first = pl.program_id(0) == 0

    @pl.when(first)
    def _():
        rows = n // len(parts)
        for rel, part in enumerate(parts):
            wd_ref[pl.ds(pl.multiple_of((chip_ref[0] ^ rel) * rows, rows), rows), :] = part[...]

    wgu, wd = wgu_ref[...], wd_ref[...]
    gu = mm(jnp.where(first, xa_ref[...], xb_ref[...]), wgu, 1, 0)
    hg = mm(jnp.where(first, ua_ref[...], ub_ref[...]), wd, 1, 1)
    gate, upper = gu[:, :n], gu[:, n:]
    sig = 1.0 / (1.0 + jnp.exp(-gate))
    act = gate * sig
    hidden = (act * upper).astype(bf16)
    hid_ref[...] = hidden
    gg = (hg * upper * sig * (1.0 + gate * (1.0 - sig))).astype(bf16)
    ug = (hg * act).astype(bf16)
    gug_ref[:, :n] = gg
    gug_ref[:, n:] = ug
    ng_ref[...] = (mm(gg, wgu[:, :n], 1, 1) + mm(ug, wgu[:, n:], 1, 1)).astype(bf16)
    out_ref[...] = mm(hidden, wd, 1, 0).astype(bf16)


def feed(xs, us, wgu, wd_parts, chip, first, blocks, into=()):
    r, d = xs[0].shape
    n = wgu.shape[1] // 2
    row = pl.BlockSpec((r, d), lambda i, _: (i, 0))
    block = lambda cols: pl.BlockSpec((r, cols), lambda i, _: (i + first, 0))
    whole = lambda a: pl.BlockSpec(a.shape, lambda i, _: (0, 0), pipeline_mode=pl.Buffered(1))
    shape = lambda rows, cols: jax.ShapeDtypeStruct((rows, cols), bf16)
    args = (*xs, *us, wgu, *wd_parts)
    k = 1 + len(args)
    body = lambda *refs: feed_kernel(*refs[:6], refs[6:k], *refs[k + len(into) :])
    return pl.pallas_call(
        body,
        grid_spec=pltpu.PrefetchScalarGridSpec(
            num_scalar_prefetch=1,
            grid=(2,),
            in_specs=[whole(a) for a in args] + [pl.BlockSpec(memory_space=pl.ANY)] * len(into),
            out_specs=[block(n), block(2 * n), row, row],
            scratch_shapes=[pltpu.VMEM((n, d), bf16)],
        ),
        out_shape=[shape(blocks * r, n), shape(blocks * r, 2 * n)] + [shape(2 * r, d)] * 2,
        input_output_aliases={k + i: i for i in range(len(into))},
        cost_estimate=pl.CostEstimate(
            flops=28 * r * d * n, bytes_accessed=2 * (8 * r * d + 6 * r * n + 3 * d * n), transcendentals=2 * r * n
        ),
        name="feed",
    )(chip[None], *args, *into)


def after(x, *deps):
    return lax.optimization_barrier((x, *deps))[0]


def row_norm(values):
    scale = lax.rsqrt(jnp.mean(values * values, axis=-1, keepdims=True) + EPS)
    return (values * scale).astype(bf16), scale


def row_norm_back(values, scale, weighted):
    inner = jnp.mean(weighted * values, axis=-1, keepdims=True)
    return scale * weighted - values * (scale * scale * scale * inner)


def build(mesh):
    F, Z = mesh.shape["fsdp"], mesh.shape["ctx"]
    C = F // 2
    assert F == 2 * C and F & (F - 1) == 0 and Z & (Z - 1) == 0 and Z > 1
    chip_bits = [2 << i for i in range(C.bit_length() - 1)]
    z_bits = [1 << i for i in range(Z.bit_length() - 1)]
    sizes = {"fsdp": F, "ctx": Z}

    def hop(x, axis, bit):
        return lax.ppermute(x, axis, [(i, i ^ bit) for i in range(sizes[axis])])

    def shift(x, by):
        return lax.ppermute(x, "ctx", [(i, i + by) for i in range(Z) if 0 <= i + by < Z])

    def place(buf, part, c, rel):
        return lax.dynamic_update_slice(buf, part, ((c ^ rel) * (buf.shape[0] // C), 0))

    def by_chip(parts, c, *deps):
        r, n = parts[0].shape
        out = after(jnp.zeros((C * r, n), parts[0].dtype), *deps)
        for rel, part in enumerate(parts):
            out = place(out, part, c, rel)
        return out

    def spread(piece):
        return [piece] + [hop(piece, "fsdp", 2 * rel) for rel in range(1, C)]

    def by_chip_copies(piece):
        return jnp.broadcast_to(piece, (C, *piece.shape))

    def exchange(copies):
        out = lax.all_to_all(copies, "fsdp", 0, 0, axis_index_groups=groups)
        return out.reshape(-1, out.shape[-1])

    groups = [[2 * i + k for i in range(C)] for k in range(2)]

    def scatter(full):
        full = full.reshape(C, -1, full.shape[-1])
        return lax.all_to_all(full, "fsdp", 0, 0, axis_index_groups=groups)

    def scatter_hops(full, c):
        r = full.shape[0] // C
        parts = [lax.dynamic_slice_in_dim(full, (c ^ rel) * r, r) for rel in range(C)]
        return [parts[0]] + [hop(parts[rel], "fsdp", 2 * rel) for rel in range(1, C)]

    def total(parts, *deps):
        if not isinstance(parts, list):
            return jnp.sum(after(parts, *deps).astype(f32), axis=0)
        return functools.reduce(lambda a, b: a + b, [after(p, *deps).astype(f32) for p in parts])

    def z_sum(b, bits):
        for bit in bits:
            b = (b.astype(f32) + hop(b, "ctx", bit).astype(f32)).astype(bf16)
        return b

    def z_sum_split(own, zb):
        h = own.shape[0] // 2
        top, bottom = own[:h], own[h:]
        mine, theirs = jnp.where(zb == 0, top, bottom), jnp.where(zb == 0, bottom, top)
        mine = mine.astype(f32) + hop(theirs.astype(bf16), "ctx", 1).astype(f32)
        b = z_sum(mine.astype(bf16), z_bits[1:])
        o = hop(b, "ctx", 1)
        return jnp.where(zb == 0, jnp.concatenate([b, o]), jnp.concatenate([o, b]))

    def body(
        tokens, segments, cotangent, attn_gain, w_query, key_matrix, value_matrix, w_out,
        query_gain, key_gain, ffn_gain, w_gate, w_up, w_down,
    ):
        me = lax.axis_index("fsdp")
        core, c = me % 2, me // 2
        zb = lax.axis_index("ctx") % 2
        R, D = tokens.shape[1:]
        hd = query_gain.shape[0]
        heads, kv_heads = w_query.shape[1] // hd, key_matrix.shape[1] // hd
        group = heads // F
        kv_split = kv_heads == F
        assert heads % F == 0 and (kv_split or (kv_heads == C and heads == F))
        halos = -(-(DOC_MAX - 1) // R)
        K = (halos + 1) * R
        qc = group * hd
        dr = w_query.shape[0]
        FS = w_down.shape[0] // 2
        swap = lambda x: hop(x, "fsdp", 1)
        by_core = lambda a, b: jnp.where(core == 0, a, b)

        where = jnp.stack([core, zb])

        def chip_rows(mine, theirs):
            got = swap(theirs)
            return by_core(jnp.concatenate([mine, got]), jnp.concatenate([got, mine]))

        mine, theirs = select_qkv(core, attn_gain[None], w_query, key_matrix, value_matrix, C, qc, hd, kv_split)
        qkv_piece = by_chip_copies(chip_rows(mine, theirs))
        qkv = exchange(qkv_piece)
        pad = 16
        seg_rows = jnp.zeros((pad, D), bf16).at[0, :R].set((segments[0] + 1).astype(bf16))
        cur = jnp.concatenate([tokens[0], seg_rows])

        gu_piece = chip_rows(*select_units(where, ffn_gain[None], after(w_gate, qkv_piece), w_up, C))
        gu_copies = by_chip_copies(gu_piece)
        d_w = after(w_down, gu_piece)
        d_piece = jnp.where(zb == 0, d_w[:FS], d_w[FS:])
        cur = after(cur, qkv_piece)
        window = [shift(cur, i) for i in range(halos, 0, -1)] + [cur]
        half = hd // 2
        freq = 1.0 / ROPE_BASE ** (jnp.arange(half, dtype=f32) * 2.0 / hd)
        angle = after(jnp.arange(K, dtype=f32), qkv_piece)[:, None] * freq[None, :]
        cosine, sine = jnp.cos(angle), jnp.sin(angle)
        window = jnp.stack(window)
        window = jnp.stack([window, swap(window)])
        seg = window[:, :, R, :R].reshape(2, K).astype(jnp.int32)
        toks = window[:, :, :R].reshape(2, K, D)
        tables = (
            jnp.concatenate([cosine, cosine], axis=1),
            jnp.concatenate([-sine, sine], axis=1),
            seg[:, K - R :, None],
            seg[:, None, :],
            query_gain.astype(f32)[None],
            key_gain.astype(f32)[None],
        )
        normed, scale_attn = row_norm(after(toks, gu_copies, tables[0], tables[1], d_piece).astype(f32))

        qkv, normed = lax.optimization_barrier((qkv, normed))
        o_parts = spread(after(w_out, qkv))

        wq, wkv = qkv[:, : C * qc], qkv[:, C * qc :]
        normed_own = normed[:, K - R :].reshape(2 * R, D)
        normed_all = normed.reshape(2 * K, D)
        kv_raw = mm(normed_all, wkv, 1, 0)
        q_raw = mm(normed_own, wq, 1, 0)
        w_gu = exchange(after(gu_copies, q_raw))
        d_parts = spread(after(d_piece, q_raw))
        context = attend(q_raw, after(kv_raw, q_raw), tables, 2, R, K, group, hd)
        context = after(context, w_gu)
        cot = after(cotangent[0], context)
        cot_z = hop(cot, "ctx", 1)
        us = [cot, swap(cot), cot_z, swap(cot_z)]
        w_o = by_chip([after(p, context) for p in o_parts], c)
        part = mm(context, w_o, 1, 0)
        middle = toks[0, K - R :].astype(f32) + part[:R] + swap(part[R:].astype(bf16)).astype(f32)

        nf, scale_ffn = row_norm(middle)
        nf_z = hop(nf, "ctx", 1)
        xs = [nf, swap(nf)]
        hidden, gug, ng_own, out_own = feed(xs, us[:2], w_gu, d_parts, c, 0, 4)
        xs += [nf_z, swap(after(nf_z, ng_own))]
        hidden, gug, ng_z, out_z = feed(xs[2:], us[2:], w_gu, d_parts, c, 2, 4, (hidden, gug))
        x4, u4 = jnp.concatenate(xs), jnp.concatenate(us)

        ng_send = (ng_z[:R].astype(f32) + swap(ng_z[R:]).astype(f32)).astype(bf16)
        ng_got = hop(ng_send, "ctx", 1)
        ng_here = ng_own[:R].astype(f32) + swap(ng_own[R:]).astype(f32)

        gu_grads = scatter(mm(after(x4, ng_send), gug, 0, 0).astype(bf16))
        down_full = mm(after(hidden, ng_send), u4, 0, 0).astype(bf16)

        normed_grad = ng_here + after(ng_got, down_full).astype(f32)
        ffn_gain_term = jnp.sum(normed_grad * middle * scale_ffn, axis=0)
        middle_grad = cotangent[0].astype(f32) + row_norm_back(middle, scale_ffn, normed_grad)

        ml = middle_grad.astype(bf16)
        ml2 = jnp.concatenate([ml, swap(ml)])
        out_send = (out_z[:R].astype(f32) + swap(after(out_z[R:], ml)).astype(f32)).astype(bf16)
        out_here = out_own[:R].astype(f32) + swap(out_own[R:]).astype(f32)
        out_got = hop(out_send, "ctx", 1)
        context_grad = mm(ml2, w_o, 1, 1).astype(bf16)
        out_full = mm(context, after(ml2, context_grad), 0, 0).astype(bf16)
        down_out = jnp.concatenate([down_full.reshape(C, -1, D), out_full.reshape(C, -1, D)], axis=1).reshape(-1, D)
        do_grads = scatter_hops(down_out, c)

        def core_rows(rows):
            top, bottom = rows[:dr], rows[dr:]
            mine, theirs = by_core(top, bottom), by_core(bottom, top)
            return mine, swap(theirs.astype(bf16)).astype(f32)

        def by_parity(mine, other):
            return by_core(mine, other), by_core(other, mine)

        cg = after(context_grad, out_send, down_out)
        dq, dkv, qgg, kgg = attend_back(q_raw, kv_raw, cg, tables, 2, R, K, group, hd)
        gu_grads = after(gu_grads, dq)
        mine, got = core_rows(total(gu_grads))
        gu_s = jnp.concatenate([mine, got]).astype(bf16)
        gu_z = z_sum(gu_s, z_bits[1:])

        q_full = mm(normed_own, after(dq, gu_s), 0, 0).astype(bf16)
        kv_full = mm(normed_all, after(dkv, gu_s), 0, 0).astype(bf16)
        qkv_grads = scatter(jnp.concatenate([q_full, kv_full], axis=1))

        do_sum = total(do_grads, q_full, kv_full, gu_z)
        zpick = lambda x: (jnp.where(zb == 0, x[0], x[1]), jnp.where(zb == 0, x[1], x[0]))
        mine, theirs = zpick(do_sum[FS:].reshape(2, -1, D))
        mine = mine + hop(theirs.astype(bf16), "ctx", 1).astype(f32)
        do_s = jnp.concatenate([do_sum[:FS], mine]).astype(bf16)
        do_z = z_sum(do_s, z_bits[1:])
        do_o = hop(do_z, "ctx", 1)
        o = hop(gu_z, "ctx", 1)

        sent = (qkv_grads, do_s)
        own_rows = mm(after(dq, *sent), wq, 1, 1)
        attn_grad = mm(after(dkv, *sent), wkv, 1, 1).reshape(2, K, D)
        attn_grad = attn_grad + jnp.pad(own_rows.reshape(2, R, D), ((0, 0), (K - R, 0), (0, 0)))
        attn_grad = attn_grad[0] + swap(attn_grad[1].astype(bf16)).astype(f32)
        attn_gain_term = jnp.sum(attn_grad * toks[0].astype(f32) * scale_attn[0], axis=0)
        carry = attn_grad[:R]
        for i in range(1, halos + 1):
            carry = after(carry, o)
            carry = attn_grad[i * R : (i + 1) * R] + shift(carry.astype(bf16), -1).astype(f32)
        input_grad = middle_grad + row_norm_back(
            toks[0, K - R :].astype(f32), scale_attn[0, K - R :], carry
        )

        small = jnp.concatenate([qgg[0], kgg[0], ffn_gain_term, attn_gain_term])
        small = small.reshape(-1, 128)
        small = small + swap(small)
        small = functools.reduce(lambda a, b: a + b, [small] + [hop(small, "fsdp", 2 * rel) for rel in range(1, C)])
        small = small.reshape(-1)
        own = lambda base: lax.dynamic_slice_in_dim(small, base + me * dr, dr)
        gains = jnp.concatenate([own(2 * hd), own(2 * hd + D), small[: 2 * hd]]).reshape(-1, 128)
        for bit in z_bits:
            gains = gains + hop(gains, "ctx", bit)
        gains = gains.reshape(-1)

        attn_rows = attn_gain.astype(f32)[:, None]
        d_gate, d_up = place_units(where, ffn_gain[None], gu_z, o, C)
        output = (middle + out_here + after(out_got, dq).astype(f32)).astype(bf16)

        mine, got = core_rows(total(qkv_grads))
        nq = C * qc
        rows = [mine[:, :nq], got[:, :nq]]
        if kv_split:
            rows += [mine[:, nq:], got[:, nq:]]
        full = z_sum_split(jnp.concatenate(rows), zb).astype(f32)
        rows = [full[i * dr : (i + 1) * dr] * attn_rows for i in range(len(rows))]
        pair = by_parity(*rows[:2])
        d_query = jnp.concatenate([p[:, i * qc : (i + 1) * qc] for i in range(C) for p in pair], axis=1)
        if kv_split:
            kv = by_parity(*rows[2:])
        else:
            kv = (z_sum_split(mine[:, nq:] + got[:, nq:], zb).astype(f32) * attn_rows,)
        pick = lambda off: jnp.concatenate(
            [p[:, 2 * i * hd + off : 2 * i * hd + off + hd] for i in range(C) for p in kv], axis=1
        )
        d_key, d_value = pick(0), pick(hd)

        both = [jnp.where(zb == 0, do_z, do_o), jnp.where(zb == 0, do_o, do_z)]
        d_down = jnp.concatenate([b[:FS] for b in both]).astype(f32)
        d_out = jnp.concatenate([b[FS:] for b in both]).astype(f32)
        d_ffn_gain = gains[:dr] / ffn_gain.astype(f32)
        d_attn_gain = gains[dr : 2 * dr] / attn_gain.astype(f32)
        head_gains = gains[2 * dr : 2 * dr + 2 * hd]
        return (
            output[None],
            input_grad[None],
            d_attn_gain,
            d_query,
            d_key,
            d_value,
            d_out,
            head_gains[:hd],
            head_gains[hd:],
            d_ffn_gain,
            d_gate,
            d_up,
            d_down,
        )

    return body


def solution(mesh):
    row = P("fsdp", None)
    token = P("fsdp", "ctx", None)
    in_specs = (token, P("fsdp", "ctx"), token, P("fsdp"), row, row, row, row, P(), P(), P("fsdp"), row, row, row)
    out_specs = (token, token, P("fsdp"), row, row, row, row, P(), P(), P("fsdp"), row, row, row)
    return jax.shard_map(build(mesh), mesh=mesh, in_specs=in_specs, out_specs=out_specs, check_vma=False)
```

```python
import functools
import math

import jax
import jax.numpy as jnp
from jax import lax
from jax.experimental import pallas as pl
from jax.experimental.pallas import tpu as pltpu
from jax.sharding import PartitionSpec as P

EPS = 1e-06
ROPE_BASE = 1000000.0
NEG = -1e30
DOC_MAX = 512
QB = 128

f32 = jnp.float32
bf16 = jnp.bfloat16


def mm(a, b, ca, cb):
    return lax.dot_general(a, b, (((ca,), (cb,)), ((), ())), preferred_element_type=f32)


def head_norm(x, gain):
    scale = lax.rsqrt(jnp.mean(x * x, axis=-1, keepdims=True) + EPS)
    return x * scale * gain, scale


def rotate(u, cosine, sine):
    return u * cosine + pltpu.roll(u, u.shape[-1] // 2, axis=1) * sine


def rotate_back(r, cosine, sine):
    return r * cosine - pltpu.roll(r, r.shape[-1] // 2, axis=1) * sine


def mask_bias(segc, segr, lo, halo, width):
    row = lax.broadcasted_iota(jnp.int32, (QB, width), 0)
    col = lax.broadcasted_iota(jnp.int32, (QB, width), 1)
    same = segc[lo : lo + QB, :] == segr[:, lo : lo + width]
    return jnp.where(same & (col <= row + halo), 0.0, NEG)


def attend_kernel(group, halo, q_ref, kv_ref, cos_ref, sin_ref, segc_ref, segr_ref, qg_ref, kg_ref, ctx_ref):
    hd = cos_ref.shape[1]
    rows = q_ref.shape[0]
    width = halo + QB
    scale = 1.0 / math.sqrt(hd)
    cosine, sine = cos_ref[...], sin_ref[...]
    kn, _ = head_norm(kv_ref[:, :hd], kg_ref[...])
    k_low = rotate(kn, cosine, sine).astype(bf16)
    v_low = kv_ref[:, hd:].astype(bf16)
    for i in range(rows // QB):
        lo = i * QB
        bias = mask_bias(segc_ref[0], segr_ref[0], lo, halo, width)
        qs = []
        for h in range(group):
            qn, _ = head_norm(q_ref[lo : lo + QB, h * hd : (h + 1) * hd], qg_ref[...])
            at = halo + lo
            qs.append(rotate(qn, cosine[at : at + QB], sine[at : at + QB]).astype(bf16))
        q_low = jnp.concatenate(qs, axis=0)
        s = mm(q_low, k_low[lo : lo + width], 1, 1)
        e = jnp.exp(s * scale + jnp.concatenate([bias] * group, axis=0))
        p = (e * (1.0 / jnp.sum(e, axis=-1, keepdims=True))).astype(bf16)
        c = mm(p, v_low[lo : lo + width], 1, 0).astype(bf16)
        for h in range(group):
            ctx_ref[lo : lo + QB, h * hd : (h + 1) * hd] = c[h * QB : (h + 1) * QB]


def attend_back_kernel(
    group, halo, q_ref, kv_ref, dc_ref, cos_ref, sin_ref, segc_ref, segr_ref, qg_ref, kg_ref,
    dq_ref, dkv_ref, qgg_ref, kgg_ref, dk_ref, dv_ref,
):
    hd = cos_ref.shape[1]
    rows = q_ref.shape[0]
    width = halo + QB
    scale = 1.0 / math.sqrt(hd)
    cosine, sine = cos_ref[...], sin_ref[...]
    q_gain, k_gain = qg_ref[...], kg_ref[...]

    @pl.when((pl.program_id(0) == 0) & (pl.program_id(1) == 0))
    def _():
        qgg_ref[...] = jnp.zeros_like(qgg_ref)
        kgg_ref[...] = jnp.zeros_like(kgg_ref)

    k_raw = kv_ref[:, :hd]
    kn, k_scale = head_norm(k_raw, k_gain)
    k_low = rotate(kn, cosine, sine).astype(bf16)
    v_low = kv_ref[:, hd:].astype(bf16)
    dk_ref[...] = jnp.zeros_like(dk_ref)
    dv_ref[...] = jnp.zeros_like(dv_ref)
    q_gain_grad = jnp.zeros((1, hd), f32)
    for i in range(rows // QB):
        lo = i * QB
        at = halo + lo
        cq, sq = cosine[at : at + QB], sine[at : at + QB]
        bias = mask_bias(segc_ref[0], segr_ref[0], lo, halo, width)
        raws, scales, lows, dcs = [], [], [], []
        for h in range(group):
            raw = q_ref[lo : lo + QB, h * hd : (h + 1) * hd]
            qn, q_scale = head_norm(raw, q_gain)
            raws.append(raw)
            scales.append(q_scale)
            lows.append(rotate(qn, cq, sq).astype(bf16))
            dcs.append(dc_ref[lo : lo + QB, h * hd : (h + 1) * hd])
        q_low = jnp.concatenate(lows, axis=0)
        dc = jnp.concatenate(dcs, axis=0)
        kw, vw = k_low[lo : lo + width], v_low[lo : lo + width]
        s = mm(q_low, kw, 1, 1)
        e = jnp.exp(s * scale + jnp.concatenate([bias] * group, axis=0))
        p = e * (1.0 / jnp.sum(e, axis=-1, keepdims=True))
        dp = mm(dc, vw, 1, 1)
        inner = jnp.sum(p * dp, axis=-1, keepdims=True)
        ds = (p * (dp - inner)).astype(bf16)
        dq = mm(ds, kw, 1, 0) * scale
        dk_ref[lo : lo + width, :] += mm(ds, q_low, 0, 0)
        dv_ref[lo : lo + width, :] += mm(p.astype(bf16), dc, 0, 0)
        for h in range(group):
            rot = rotate_back(dq[h * QB : (h + 1) * QB], cq, sq)
            raw, sc = raws[h], scales[h]
            b = rot * q_gain
            q_gain_grad += jnp.sum(rot * raw * sc, axis=0, keepdims=True)
            grad = sc * b - raw * (sc * sc * sc * jnp.mean(b * raw, axis=-1, keepdims=True))
            dq_ref[lo : lo + QB, h * hd : (h + 1) * hd] = grad.astype(bf16)
    qgg_ref[...] += q_gain_grad
    rot = rotate_back(dk_ref[...] * scale, cosine, sine)
    b = rot * k_gain
    kgg_ref[...] += jnp.sum(rot * k_raw * k_scale, axis=0, keepdims=True)
    grad = k_scale * b - k_raw * (k_scale * k_scale * k_scale * jnp.mean(b * k_raw, axis=-1, keepdims=True))
    dkv_ref[:, :hd] = grad.astype(bf16)
    dkv_ref[:, hd:] = dv_ref[...].astype(bf16)


def attention_specs(seqs, rows, keys, group, hd):
    return [
        pl.BlockSpec((rows, group * hd), lambda j, g: (j, g)),
        pl.BlockSpec((keys, 2 * hd), lambda j, g: (j, g)),
    ], [
        pl.BlockSpec((keys, hd), lambda j, g: (0, 0)),
        pl.BlockSpec((keys, hd), lambda j, g: (0, 0)),
        pl.BlockSpec((1, rows, 1), lambda j, g: (j, 0, 0)),
        pl.BlockSpec((1, 1, keys), lambda j, g: (j, 0, 0)),
        pl.BlockSpec((1, hd), lambda j, g: (0, 0)),
        pl.BlockSpec((1, hd), lambda j, g: (0, 0)),
    ]


def attend(q_raw, kv_raw, tables, seqs, rows, keys, group, hd):
    heads = kv_raw.shape[1] // (2 * hd)
    first, rest = attention_specs(seqs, rows, keys, group, hd)
    pairs = seqs * heads * group * rows * (keys - rows + QB)
    return pl.pallas_call(
        functools.partial(attend_kernel, group, keys - rows),
        grid=(seqs, heads),
        in_specs=first + rest,
        out_specs=pl.BlockSpec((rows, group * hd), lambda j, g: (j, g)),
        out_shape=jax.ShapeDtypeStruct(q_raw.shape, bf16),
        cost_estimate=pl.CostEstimate(
            flops=4 * pairs * hd, bytes_accessed=q_raw.size * 6 + kv_raw.size * 4, transcendentals=pairs
        ),
        compiler_params=pltpu.CompilerParams(vmem_limit_bytes=20 << 20),
        name="attend",
    )(q_raw, kv_raw, *tables)


def attend_back(q_raw, kv_raw, context_grad, tables, seqs, rows, keys, group, hd):
    heads = kv_raw.shape[1] // (2 * hd)
    first, rest = attention_specs(seqs, rows, keys, group, hd)
    pairs = seqs * heads * group * rows * (keys - rows + QB)
    gain_spec = pl.BlockSpec((1, hd), lambda j, g: (0, 0))
    return pl.pallas_call(
        functools.partial(attend_back_kernel, group, keys - rows),
        grid=(seqs, heads),
        in_specs=first + [first[0]] + rest,
        out_specs=[first[0], first[1], gain_spec, gain_spec],
        out_shape=[
            jax.ShapeDtypeStruct(q_raw.shape, bf16),
            jax.ShapeDtypeStruct(kv_raw.shape, bf16),
            jax.ShapeDtypeStruct((1, hd), f32),
            jax.ShapeDtypeStruct((1, hd), f32),
        ],
        scratch_shapes=[pltpu.VMEM((keys, hd), f32), pltpu.VMEM((keys, hd), f32)],
        cost_estimate=pl.CostEstimate(
            flops=10 * pairs * hd,
            bytes_accessed=seqs * heads * (8 * rows * group * hd + 12 * keys * hd),
            transcendentals=pairs,
        ),
        compiler_params=pltpu.CompilerParams(vmem_limit_bytes=28 << 20),
        name="attend_back",
    )(q_raw, kv_raw, context_grad, *tables)


def diagonal(gain_ref):
    n = gain_ref.shape[1]
    row = lax.broadcasted_iota(jnp.int32, (n, n), 0)
    col = lax.broadcasted_iota(jnp.int32, (n, n), 1)
    return jnp.where(row == col, gain_ref[...].astype(f32), 0.0).astype(bf16)


def select_kernel(chips, qc, hd, split, core_ref, gain_ref, wq_ref, wk_ref, wv_ref, mine_ref, theirs_ref):
    gain = diagonal(gain_ref)
    for out_ref, k in ((mine_ref, core_ref[0]), (theirs_ref, 1 - core_ref[0])):
        for i in range(chips):
            at = pl.ds(pl.multiple_of((2 * i + k) * qc, qc), qc)
            out_ref[:, i * qc : (i + 1) * qc] = mm(gain, wq_ref[:, at], 1, 0).astype(bf16)
            at = pl.ds(pl.multiple_of((2 * i + k if split else i) * hd, hd), hd)
            base = chips * qc + 2 * i * hd
            out_ref[:, base : base + hd] = mm(gain, wk_ref[:, at], 1, 0).astype(bf16)
            out_ref[:, base + hd : base + 2 * hd] = mm(gain, wv_ref[:, at], 1, 0).astype(bf16)


def small_call(kernel, scalars, args, outs, name):
    spec = lambda a: pl.BlockSpec(a.shape, lambda i, *_: (0,) * len(a.shape), pipeline_mode=pl.Buffered(1))
    size = lambda a: math.prod(a.shape) * a.dtype.itemsize
    return pl.pallas_call(
        kernel,
        grid_spec=pltpu.PrefetchScalarGridSpec(
            num_scalar_prefetch=1,
            grid=(1,),
            in_specs=[spec(a) for a in args],
            out_specs=[spec(o) for o in outs],
        ),
        out_shape=outs,
        cost_estimate=pl.CostEstimate(
            flops=0, bytes_accessed=sum(size(a) for a in (*args, *outs)), transcendentals=0
        ),
        compiler_params=pltpu.CompilerParams(vmem_limit_bytes=16 << 20),
        name=name,
    )(scalars, *args)


def select_qkv(core, gain, wq, wk, wv, chips, qc, hd, split):
    out = jax.ShapeDtypeStruct((wq.shape[0], chips * (qc + 2 * hd)), bf16)
    kernel = functools.partial(select_kernel, chips, qc, hd, split)
    return small_call(kernel, core[None], (gain, wq, wk, wv), (out, out), "select_qkv")


def select_units_kernel(chips, where_ref, gain_ref, wg_ref, wu_ref, mine_ref, theirs_ref):
    n = wg_ref.shape[1] // (4 * chips)
    gain = diagonal(gain_ref)
    for k in range(2):
        for z in range(2):

            @pl.when((where_ref[0] == k) & (where_ref[1] == z))
            def _():
                for out_ref, kk in ((mine_ref, k), (theirs_ref, 1 - k)):
                    for m, w_ref in enumerate((wg_ref, wu_ref)):
                        cols = [w_ref[:, (4 * i + 2 * kk + z) * n : (4 * i + 2 * kk + z + 1) * n] for i in range(chips)]
                        out = mm(gain, jnp.concatenate(cols, axis=1), 1, 0)
                        out_ref[:, m * chips * n : (m + 1) * chips * n] = out.astype(bf16)


def select_units(where, gain, wg, wu, chips):
    out = jax.ShapeDtypeStruct((wg.shape[0], wg.shape[1] // 2), bf16)
    kernel = functools.partial(select_units_kernel, chips)
    return small_call(kernel, where, (gain, wg, wu), (out, out), "select_units")


def place_units_kernel(chips, where_ref, gain_ref, a_ref, b_ref, dg_ref, du_ref):
    dr = dg_ref.shape[0]
    n = dg_ref.shape[1] // (4 * chips)
    gain = diagonal(gain_ref)
    for k in range(2):
        for z in range(2):

            @pl.when((where_ref[0] == k) & (where_ref[1] == z))
            def _():
                for m, out_ref in enumerate((dg_ref, du_ref)):
                    for i in range(chips):
                        cols = []
                        for kk in range(2):
                            for zz in range(2):
                                ref = a_ref if zz == z else b_ref
                                top = 0 if kk == k else dr
                                at = (m * chips + i) * n
                                cols.append(ref[top : top + dr, at : at + n])
                        out_ref[:, 4 * i * n : 4 * (i + 1) * n] = mm(gain, jnp.concatenate(cols, axis=1), 1, 0)


def place_units(where, gain, a, b, chips):
    out = jax.ShapeDtypeStruct((a.shape[0] // 2, 2 * a.shape[1]), f32)
    kernel = functools.partial(place_units_kernel, chips)
    return small_call(kernel, where, (gain, a, b), (out, out), "place_units")


def feed_kernel(chip_ref, xa_ref, xb_ref, ua_ref, ub_ref, wgu_ref, parts, hid_ref, gug_ref, ng_ref, out_ref, wd_ref):
    n = wd_ref.shape[0]
    first = pl.program_id(0) == 0

    @pl.when(first)
    def _():
        rows = n // len(parts)
        for rel, part in enumerate(parts):
            wd_ref[pl.ds(pl.multiple_of((chip_ref[0] ^ rel) * rows, rows), rows), :] = part[...]

    wgu, wd = wgu_ref[...], wd_ref[...]
    gu = mm(jnp.where(first, xa_ref[...], xb_ref[...]), wgu, 1, 0)
    hg = mm(jnp.where(first, ua_ref[...], ub_ref[...]), wd, 1, 1)
    gate, upper = gu[:, :n], gu[:, n:]
    sig = 1.0 / (1.0 + jnp.exp(-gate))
    act = gate * sig
    hidden = (act * upper).astype(bf16)
    hid_ref[...] = hidden
    gg = (hg * upper * sig * (1.0 + gate * (1.0 - sig))).astype(bf16)
    ug = (hg * act).astype(bf16)
    gug_ref[:, :n] = gg
    gug_ref[:, n:] = ug
    ng_ref[...] = (mm(gg, wgu[:, :n], 1, 1) + mm(ug, wgu[:, n:], 1, 1)).astype(bf16)
    out_ref[...] = mm(hidden, wd, 1, 0).astype(bf16)


def feed(xs, us, wgu, wd_parts, chip, first, blocks, into=()):
    r, d = xs[0].shape
    n = wgu.shape[1] // 2
    row = pl.BlockSpec((r, d), lambda i, _: (i, 0))
    block = lambda cols: pl.BlockSpec((r, cols), lambda i, _: (i + first, 0))
    whole = lambda a: pl.BlockSpec(a.shape, lambda i, _: (0, 0), pipeline_mode=pl.Buffered(1))
    shape = lambda rows, cols: jax.ShapeDtypeStruct((rows, cols), bf16)
    args = (*xs, *us, wgu, *wd_parts)
    k = 1 + len(args)
    body = lambda *refs: feed_kernel(*refs[:6], refs[6:k], *refs[k + len(into) :])
    return pl.pallas_call(
        body,
        grid_spec=pltpu.PrefetchScalarGridSpec(
            num_scalar_prefetch=1,
            grid=(2,),
            in_specs=[whole(a) for a in args] + [pl.BlockSpec(memory_space=pl.ANY)] * len(into),
            out_specs=[block(n), block(2 * n), row, row],
            scratch_shapes=[pltpu.VMEM((n, d), bf16)],
        ),
        out_shape=[shape(blocks * r, n), shape(blocks * r, 2 * n)] + [shape(2 * r, d)] * 2,
        input_output_aliases={k + i: i for i in range(len(into))},
        cost_estimate=pl.CostEstimate(
            flops=28 * r * d * n, bytes_accessed=2 * (8 * r * d + 6 * r * n + 3 * d * n), transcendentals=2 * r * n
        ),
        name="feed",
    )(chip[None], *args, *into)


def after(x, *deps):
    return lax.optimization_barrier((x, *deps))[0]


def row_norm(values):
    scale = lax.rsqrt(jnp.mean(values * values, axis=-1, keepdims=True) + EPS)
    return (values * scale).astype(bf16), scale


def row_norm_back(values, scale, weighted):
    inner = jnp.mean(weighted * values, axis=-1, keepdims=True)
    return scale * weighted - values * (scale * scale * scale * inner)


def build(mesh):
    F, Z = mesh.shape["fsdp"], mesh.shape["ctx"]
    C = F // 2
    assert F == 2 * C and F & (F - 1) == 0 and Z & (Z - 1) == 0 and Z > 1
    chip_bits = [2 << i for i in range(C.bit_length() - 1)]
    z_bits = [1 << i for i in range(Z.bit_length() - 1)]
    sizes = {"fsdp": F, "ctx": Z}

    def hop(x, axis, bit):
        return lax.ppermute(x, axis, [(i, i ^ bit) for i in range(sizes[axis])])

    def shift(x, by):
        return lax.ppermute(x, "ctx", [(i, i + by) for i in range(Z) if 0 <= i + by < Z])

    def place(buf, part, c, rel):
        return lax.dynamic_update_slice(buf, part, ((c ^ rel) * (buf.shape[0] // C), 0))

    def by_chip(parts, c, *deps):
        r, n = parts[0].shape
        out = after(jnp.zeros((C * r, n), parts[0].dtype), *deps)
        for rel, part in enumerate(parts):
            out = place(out, part, c, rel)
        return out

    def spread(piece):
        return [piece] + [hop(piece, "fsdp", 2 * rel) for rel in range(1, C)]

    def by_chip_copies(piece):
        return jnp.broadcast_to(piece, (C, *piece.shape))

    def exchange(copies):
        out = lax.all_to_all(copies, "fsdp", 0, 0, axis_index_groups=groups)
        return out.reshape(-1, out.shape[-1])

    groups = [[2 * i + k for i in range(C)] for k in range(2)]

    def scatter(full):
        full = full.reshape(C, -1, full.shape[-1])
        return lax.all_to_all(full, "fsdp", 0, 0, axis_index_groups=groups)

    def scatter_hops(full, c):
        r = full.shape[0] // C
        parts = [lax.dynamic_slice_in_dim(full, (c ^ rel) * r, r) for rel in range(C)]
        return [parts[0]] + [hop(parts[rel], "fsdp", 2 * rel) for rel in range(1, C)]

    def total(parts, *deps):
        if not isinstance(parts, list):
            return jnp.sum(after(parts, *deps).astype(f32), axis=0)
        return functools.reduce(lambda a, b: a + b, [after(p, *deps).astype(f32) for p in parts])

    def z_sum(b, bits):
        for bit in bits:
            b = (b.astype(f32) + hop(b, "ctx", bit).astype(f32)).astype(bf16)
        return b

    def z_sum_split(own, zb):
        h = own.shape[0] // 2
        top, bottom = own[:h], own[h:]
        mine, theirs = jnp.where(zb == 0, top, bottom), jnp.where(zb == 0, bottom, top)
        mine = mine.astype(f32) + hop(theirs.astype(bf16), "ctx", 1).astype(f32)
        b = z_sum(mine.astype(bf16), z_bits[1:])
        o = hop(b, "ctx", 1)
        return jnp.where(zb == 0, jnp.concatenate([b, o]), jnp.concatenate([o, b]))

    def body(
        tokens, segments, cotangent, attn_gain, w_query, key_matrix, value_matrix, w_out,
        query_gain, key_gain, ffn_gain, w_gate, w_up, w_down,
    ):
        me = lax.axis_index("fsdp")
        core, c = me % 2, me // 2
        zb = lax.axis_index("ctx") % 2
        R, D = tokens.shape[1:]
        hd = query_gain.shape[0]
        heads, kv_heads = w_query.shape[1] // hd, key_matrix.shape[1] // hd
        group = heads // F
        kv_split = kv_heads == F
        assert heads % F == 0 and (kv_split or (kv_heads == C and heads == F))
        halos = -(-(DOC_MAX - 1) // R)
        K = (halos + 1) * R
        qc = group * hd
        dr = w_query.shape[0]
        FS = w_down.shape[0] // 2
        swap = lambda x: hop(x, "fsdp", 1)
        by_core = lambda a, b: jnp.where(core == 0, a, b)

        where = jnp.stack([core, zb])

        def chip_rows(mine, theirs):
            got = swap(theirs)
            return by_core(jnp.concatenate([mine, got]), jnp.concatenate([got, mine]))

        mine, theirs = select_qkv(core, attn_gain[None], w_query, key_matrix, value_matrix, C, qc, hd, kv_split)
        qkv_piece = by_chip_copies(chip_rows(mine, theirs))
        qkv = exchange(qkv_piece)
        pad = 16
        seg_rows = jnp.zeros((pad, D), bf16).at[0, :R].set((segments[0] + 1).astype(bf16))
        cur = jnp.concatenate([tokens[0], seg_rows])

        gu_piece = chip_rows(*select_units(where, ffn_gain[None], after(w_gate, qkv_piece), w_up, C))
        gu_copies = by_chip_copies(gu_piece)
        d_w = after(w_down, gu_piece)
        d_piece = jnp.where(zb == 0, d_w[:FS], d_w[FS:])
        cur = after(cur, qkv_piece)
        window = [shift(cur, i) for i in range(halos, 0, -1)] + [cur]
        half = hd // 2
        freq = 1.0 / ROPE_BASE ** (jnp.arange(half, dtype=f32) * 2.0 / hd)
        angle = after(jnp.arange(K, dtype=f32), qkv_piece)[:, None] * freq[None, :]
        cosine, sine = jnp.cos(angle), jnp.sin(angle)
        window = jnp.stack(window)
        window = jnp.stack([window, swap(window)])
        seg = window[:, :, R, :R].reshape(2, K).astype(jnp.int32)
        toks = window[:, :, :R].reshape(2, K, D)
        tables = (
            jnp.concatenate([cosine, cosine], axis=1),
            jnp.concatenate([-sine, sine], axis=1),
            seg[:, K - R :, None],
            seg[:, None, :],
            query_gain.astype(f32)[None],
            key_gain.astype(f32)[None],
        )
        normed, scale_attn = row_norm(after(toks, gu_copies, tables[0], tables[1], d_piece).astype(f32))

        qkv, normed = lax.optimization_barrier((qkv, normed))
        o_parts = spread(after(w_out, qkv))

        wq, wkv = qkv[:, : C * qc], qkv[:, C * qc :]
        normed_own = normed[:, K - R :].reshape(2 * R, D)
        normed_all = normed.reshape(2 * K, D)
        kv_raw = mm(normed_all, wkv, 1, 0)
        q_raw = mm(normed_own, wq, 1, 0)
        w_gu = exchange(after(gu_copies, q_raw))
        d_parts = spread(after(d_piece, q_raw))
        context = attend(q_raw, after(kv_raw, q_raw), tables, 2, R, K, group, hd)
        context = after(context, w_gu)
        cot = after(cotangent[0], context)
        cot_z = hop(cot, "ctx", 1)
        us = [cot, swap(cot), cot_z, swap(cot_z)]
        w_o = by_chip([after(p, context) for p in o_parts], c)
        part = mm(context, w_o, 1, 0)
        middle = toks[0, K - R :].astype(f32) + part[:R] + swap(part[R:].astype(bf16)).astype(f32)

        nf, scale_ffn = row_norm(middle)
        nf_z = hop(nf, "ctx", 1)
        xs = [nf, swap(nf)]
        hidden, gug, ng_own, out_own = feed(xs, us[:2], w_gu, d_parts, c, 0, 4)
        xs += [nf_z, swap(after(nf_z, ng_own))]
        hidden, gug, ng_z, out_z = feed(xs[2:], us[2:], w_gu, d_parts, c, 2, 4, (hidden, gug))
        x4, u4 = jnp.concatenate(xs), jnp.concatenate(us)

        ng_send = (ng_z[:R].astype(f32) + swap(ng_z[R:]).astype(f32)).astype(bf16)
        ng_got = hop(ng_send, "ctx", 1)
        ng_here = ng_own[:R].astype(f32) + swap(ng_own[R:]).astype(f32)

        gu_grads = scatter(mm(after(x4, ng_send), gug, 0, 0).astype(bf16))
        down_full = mm(after(hidden, ng_send), u4, 0, 0).astype(bf16)

        normed_grad = ng_here + after(ng_got, down_full).astype(f32)
        ffn_gain_term = jnp.sum(normed_grad * middle * scale_ffn, axis=0)
        middle_grad = cotangent[0].astype(f32) + row_norm_back(middle, scale_ffn, normed_grad)

        ml = middle_grad.astype(bf16)
        ml2 = jnp.concatenate([ml, swap(ml)])
        out_send = (out_z[:R].astype(f32) + swap(after(out_z[R:], ml)).astype(f32)).astype(bf16)
        out_here = out_own[:R].astype(f32) + swap(out_own[R:]).astype(f32)
        out_got = hop(out_send, "ctx", 1)
        context_grad = mm(ml2, w_o, 1, 1).astype(bf16)
        out_full = mm(context, after(ml2, context_grad), 0, 0).astype(bf16)
        down_out = jnp.concatenate([down_full.reshape(C, -1, D), out_full.reshape(C, -1, D)], axis=1).reshape(-1, D)
        do_grads = scatter_hops(down_out, c)

        def core_rows(rows):
            top, bottom = rows[:dr], rows[dr:]
            mine, theirs = by_core(top, bottom), by_core(bottom, top)
            return mine, swap(theirs.astype(bf16)).astype(f32)

        def by_parity(mine, other):
            return by_core(mine, other), by_core(other, mine)

        cg = after(context_grad, out_send, down_out)
        dq, dkv, qgg, kgg = attend_back(q_raw, kv_raw, cg, tables, 2, R, K, group, hd)
        gu_grads = after(gu_grads, dq)
        mine, got = core_rows(total(gu_grads))
        gu_s = jnp.concatenate([mine, got]).astype(bf16)
        gu_z = z_sum(gu_s, z_bits[1:])

        q_full = mm(normed_own, after(dq, gu_s), 0, 0).astype(bf16)
        kv_full = mm(normed_all, after(dkv, gu_s), 0, 0).astype(bf16)
        qkv_grads = scatter(jnp.concatenate([q_full, kv_full], axis=1))

        do_sum = total(do_grads, q_full, kv_full, gu_z)
        zpick = lambda x: (jnp.where(zb == 0, x[0], x[1]), jnp.where(zb == 0, x[1], x[0]))
        mine, theirs = zpick(do_sum[FS:].reshape(2, -1, D))
        mine = mine + hop(theirs.astype(bf16), "ctx", 1).astype(f32)
        do_s = jnp.concatenate([do_sum[:FS], mine]).astype(bf16)
        do_z = z_sum(do_s, z_bits[1:])
        do_o = hop(do_z, "ctx", 1)
        o = hop(gu_z, "ctx", 1)

        sent = (do_s,)
        own_rows = mm(after(dq, *sent), wq, 1, 1)
        attn_grad = mm(after(dkv, *sent), wkv, 1, 1).reshape(2, K, D)
        attn_grad = attn_grad + jnp.pad(own_rows.reshape(2, R, D), ((0, 0), (K - R, 0), (0, 0)))
        attn_grad = attn_grad[0] + swap(after(attn_grad[1].astype(bf16), qkv_grads)).astype(f32)
        attn_gain_term = jnp.sum(attn_grad * toks[0].astype(f32) * scale_attn[0], axis=0)
        carry = attn_grad[:R]
        for i in range(1, halos + 1):
            carry = attn_grad[i * R : (i + 1) * R] + shift(carry.astype(bf16), -1).astype(f32)
        input_grad = middle_grad + row_norm_back(
            toks[0, K - R :].astype(f32), scale_attn[0, K - R :], carry
        )

        small = jnp.concatenate([qgg[0], kgg[0], ffn_gain_term, attn_gain_term])
        small = small.reshape(-1, 128)
        small = small + swap(small)
        small = functools.reduce(lambda a, b: a + b, [small] + [hop(small, "fsdp", 2 * rel) for rel in range(1, C)])
        small = small.reshape(-1)
        own = lambda base: lax.dynamic_slice_in_dim(small, base + me * dr, dr)
        gains = jnp.concatenate([own(2 * hd), own(2 * hd + D), small[: 2 * hd]]).reshape(-1, 128)
        for bit in z_bits:
            gains = gains + hop(gains, "ctx", bit)
        gains = gains.reshape(-1)

        attn_rows = attn_gain.astype(f32)[:, None]
        d_gate, d_up = place_units(where, ffn_gain[None], gu_z, o, C)
        output = (middle + out_here + after(out_got, dq).astype(f32)).astype(bf16)

        mine, got = core_rows(total(qkv_grads))
        nq = C * qc
        rows = [mine[:, :nq], got[:, :nq]]
        if kv_split:
            rows += [mine[:, nq:], got[:, nq:]]
        full = z_sum_split(jnp.concatenate(rows), zb).astype(f32)
        rows = [full[i * dr : (i + 1) * dr] * attn_rows for i in range(len(rows))]
        pair = by_parity(*rows[:2])
        d_query = jnp.concatenate([p[:, i * qc : (i + 1) * qc] for i in range(C) for p in pair], axis=1)
        if kv_split:
            kv = by_parity(*rows[2:])
        else:
            kv = (z_sum_split(mine[:, nq:] + got[:, nq:], zb).astype(f32) * attn_rows,)
        pick = lambda off: jnp.concatenate(
            [p[:, 2 * i * hd + off : 2 * i * hd + off + hd] for i in range(C) for p in kv], axis=1
        )
        d_key, d_value = pick(0), pick(hd)

        both = [jnp.where(zb == 0, do_z, do_o), jnp.where(zb == 0, do_o, do_z)]
        d_down = jnp.concatenate([b[:FS] for b in both]).astype(f32)
        d_out = jnp.concatenate([b[FS:] for b in both]).astype(f32)
        d_ffn_gain = gains[:dr] / ffn_gain.astype(f32)
        d_attn_gain = gains[dr : 2 * dr] / attn_gain.astype(f32)
        head_gains = gains[2 * dr : 2 * dr + 2 * hd]
        return (
            output[None],
            input_grad[None],
            d_attn_gain,
            d_query,
            d_key,
            d_value,
            d_out,
            head_gains[:hd],
            head_gains[hd:],
            d_ffn_gain,
            d_gate,
            d_up,
            d_down,
        )

    return body


def solution(mesh):
    row = P("fsdp", None)
    token = P("fsdp", "ctx", None)
    in_specs = (token, P("fsdp", "ctx"), token, P("fsdp"), row, row, row, row, P(), P(), P("fsdp"), row, row, row)
    out_specs = (token, token, P("fsdp"), row, row, row, row, P(), P(), P("fsdp"), row, row, row)
    return jax.shard_map(build(mesh), mesh=mesh, in_specs=in_specs, out_specs=out_specs, check_vma=False)
```

```python
import functools
import math

import jax
import jax.numpy as jnp
from jax import lax
from jax.experimental import pallas as pl
from jax.experimental.pallas import tpu as pltpu
from jax.sharding import PartitionSpec as P

EPS = 1e-06
ROPE_BASE = 1000000.0
NEG = -1e30
DOC_MAX = 512
QB = 128

f32 = jnp.float32
bf16 = jnp.bfloat16


def mm(a, b, ca, cb):
    return lax.dot_general(a, b, (((ca,), (cb,)), ((), ())), preferred_element_type=f32)


def head_norm(x, gain):
    scale = lax.rsqrt(jnp.mean(x * x, axis=-1, keepdims=True) + EPS)
    return x * scale * gain, scale


def rotate(u, cosine, sine):
    return u * cosine + pltpu.roll(u, u.shape[-1] // 2, axis=1) * sine


def rotate_back(r, cosine, sine):
    return r * cosine - pltpu.roll(r, r.shape[-1] // 2, axis=1) * sine


def mask_bias(segc, segr, lo, halo, width):
    row = lax.broadcasted_iota(jnp.int32, (QB, width), 0)
    col = lax.broadcasted_iota(jnp.int32, (QB, width), 1)
    same = segc[lo : lo + QB, :] == segr[:, lo : lo + width]
    return jnp.where(same & (col <= row + halo), 0.0, NEG)


def attend_kernel(group, halo, q_ref, kv_ref, cos_ref, sin_ref, segc_ref, segr_ref, qg_ref, kg_ref, ctx_ref):
    hd = cos_ref.shape[1]
    rows = q_ref.shape[0]
    width = halo + QB
    scale = 1.0 / math.sqrt(hd)
    cosine, sine = cos_ref[...], sin_ref[...]
    kn, _ = head_norm(kv_ref[:, :hd], kg_ref[...])
    k_low = rotate(kn, cosine, sine).astype(bf16)
    v_low = kv_ref[:, hd:].astype(bf16)
    for i in range(rows // QB):
        lo = i * QB
        bias = mask_bias(segc_ref[0], segr_ref[0], lo, halo, width)
        qs = []
        for h in range(group):
            qn, _ = head_norm(q_ref[lo : lo + QB, h * hd : (h + 1) * hd], qg_ref[...])
            at = halo + lo
            qs.append(rotate(qn, cosine[at : at + QB], sine[at : at + QB]).astype(bf16))
        q_low = jnp.concatenate(qs, axis=0)
        s = mm(q_low, k_low[lo : lo + width], 1, 1)
        e = jnp.exp(s * scale + jnp.concatenate([bias] * group, axis=0))
        p = (e * (1.0 / jnp.sum(e, axis=-1, keepdims=True))).astype(bf16)
        c = mm(p, v_low[lo : lo + width], 1, 0).astype(bf16)
        for h in range(group):
            ctx_ref[lo : lo + QB, h * hd : (h + 1) * hd] = c[h * QB : (h + 1) * QB]


def attend_back_kernel(
    group, halo, q_ref, kv_ref, dc_ref, cos_ref, sin_ref, segc_ref, segr_ref, qg_ref, kg_ref,
    dq_ref, dkv_ref, qgg_ref, kgg_ref, dk_ref, dv_ref,
):
    hd = cos_ref.shape[1]
    rows = q_ref.shape[0]
    width = halo + QB
    scale = 1.0 / math.sqrt(hd)
    cosine, sine = cos_ref[...], sin_ref[...]
    q_gain, k_gain = qg_ref[...], kg_ref[...]

    @pl.when((pl.program_id(0) == 0) & (pl.program_id(1) == 0))
    def _():
        qgg_ref[...] = jnp.zeros_like(qgg_ref)
        kgg_ref[...] = jnp.zeros_like(kgg_ref)

    k_raw = kv_ref[:, :hd]
    kn, k_scale = head_norm(k_raw, k_gain)
    k_low = rotate(kn, cosine, sine).astype(bf16)
    v_low = kv_ref[:, hd:].astype(bf16)
    dk_ref[...] = jnp.zeros_like(dk_ref)
    dv_ref[...] = jnp.zeros_like(dv_ref)
    q_gain_grad = jnp.zeros((1, hd), f32)
    for i in range(rows // QB):
        lo = i * QB
        at = halo + lo
        cq, sq = cosine[at : at + QB], sine[at : at + QB]
        bias = mask_bias(segc_ref[0], segr_ref[0], lo, halo, width)
        raws, scales, lows, dcs = [], [], [], []
        for h in range(group):
            raw = q_ref[lo : lo + QB, h * hd : (h + 1) * hd]
            qn, q_scale = head_norm(raw, q_gain)
            raws.append(raw)
            scales.append(q_scale)
            lows.append(rotate(qn, cq, sq).astype(bf16))
            dcs.append(dc_ref[lo : lo + QB, h * hd : (h + 1) * hd])
        q_low = jnp.concatenate(lows, axis=0)
        dc = jnp.concatenate(dcs, axis=0)
        kw, vw = k_low[lo : lo + width], v_low[lo : lo + width]
        s = mm(q_low, kw, 1, 1)
        e = jnp.exp(s * scale + jnp.concatenate([bias] * group, axis=0))
        p = e * (1.0 / jnp.sum(e, axis=-1, keepdims=True))
        dp = mm(dc, vw, 1, 1)
        inner = jnp.sum(p * dp, axis=-1, keepdims=True)
        ds = (p * (dp - inner)).astype(bf16)
        dq = mm(ds, kw, 1, 0) * scale
        dk_ref[lo : lo + width, :] += mm(ds, q_low, 0, 0)
        dv_ref[lo : lo + width, :] += mm(p.astype(bf16), dc, 0, 0)
        for h in range(group):
            rot = rotate_back(dq[h * QB : (h + 1) * QB], cq, sq)
            raw, sc = raws[h], scales[h]
            b = rot * q_gain
            q_gain_grad += jnp.sum(rot * raw * sc, axis=0, keepdims=True)
            grad = sc * b - raw * (sc * sc * sc * jnp.mean(b * raw, axis=-1, keepdims=True))
            dq_ref[lo : lo + QB, h * hd : (h + 1) * hd] = grad.astype(bf16)
    qgg_ref[...] += q_gain_grad
    rot = rotate_back(dk_ref[...] * scale, cosine, sine)
    b = rot * k_gain
    kgg_ref[...] += jnp.sum(rot * k_raw * k_scale, axis=0, keepdims=True)
    grad = k_scale * b - k_raw * (k_scale * k_scale * k_scale * jnp.mean(b * k_raw, axis=-1, keepdims=True))
    dkv_ref[:, :hd] = grad.astype(bf16)
    dkv_ref[:, hd:] = dv_ref[...].astype(bf16)


def attention_specs(seqs, rows, keys, group, hd):
    return [
        pl.BlockSpec((rows, group * hd), lambda j, g: (j, g)),
        pl.BlockSpec((keys, 2 * hd), lambda j, g: (j, g)),
    ], [
        pl.BlockSpec((keys, hd), lambda j, g: (0, 0)),
        pl.BlockSpec((keys, hd), lambda j, g: (0, 0)),
        pl.BlockSpec((1, rows, 1), lambda j, g: (j, 0, 0)),
        pl.BlockSpec((1, 1, keys), lambda j, g: (j, 0, 0)),
        pl.BlockSpec((1, hd), lambda j, g: (0, 0)),
        pl.BlockSpec((1, hd), lambda j, g: (0, 0)),
    ]


def attend(q_raw, kv_raw, tables, seqs, rows, keys, group, hd):
    heads = kv_raw.shape[1] // (2 * hd)
    first, rest = attention_specs(seqs, rows, keys, group, hd)
    pairs = seqs * heads * group * rows * (keys - rows + QB)
    return pl.pallas_call(
        functools.partial(attend_kernel, group, keys - rows),
        grid=(seqs, heads),
        in_specs=first + rest,
        out_specs=pl.BlockSpec((rows, group * hd), lambda j, g: (j, g)),
        out_shape=jax.ShapeDtypeStruct(q_raw.shape, bf16),
        cost_estimate=pl.CostEstimate(
            flops=4 * pairs * hd, bytes_accessed=q_raw.size * 6 + kv_raw.size * 4, transcendentals=pairs
        ),
        compiler_params=pltpu.CompilerParams(vmem_limit_bytes=20 << 20),
        name="attend",
    )(q_raw, kv_raw, *tables)


def attend_back(q_raw, kv_raw, context_grad, tables, seqs, rows, keys, group, hd):
    heads = kv_raw.shape[1] // (2 * hd)
    first, rest = attention_specs(seqs, rows, keys, group, hd)
    pairs = seqs * heads * group * rows * (keys - rows + QB)
    gain_spec = pl.BlockSpec((1, hd), lambda j, g: (0, 0))
    return pl.pallas_call(
        functools.partial(attend_back_kernel, group, keys - rows),
        grid=(seqs, heads),
        in_specs=first + [first[0]] + rest,
        out_specs=[first[0], first[1], gain_spec, gain_spec],
        out_shape=[
            jax.ShapeDtypeStruct(q_raw.shape, bf16),
            jax.ShapeDtypeStruct(kv_raw.shape, bf16),
            jax.ShapeDtypeStruct((1, hd), f32),
            jax.ShapeDtypeStruct((1, hd), f32),
        ],
        scratch_shapes=[pltpu.VMEM((keys, hd), f32), pltpu.VMEM((keys, hd), f32)],
        cost_estimate=pl.CostEstimate(
            flops=10 * pairs * hd,
            bytes_accessed=seqs * heads * (8 * rows * group * hd + 12 * keys * hd),
            transcendentals=pairs,
        ),
        compiler_params=pltpu.CompilerParams(vmem_limit_bytes=28 << 20),
        name="attend_back",
    )(q_raw, kv_raw, context_grad, *tables)


def diagonal(gain_ref):
    n = gain_ref.shape[1]
    row = lax.broadcasted_iota(jnp.int32, (n, n), 0)
    col = lax.broadcasted_iota(jnp.int32, (n, n), 1)
    return jnp.where(row == col, gain_ref[...].astype(f32), 0.0).astype(bf16)


def select_kernel(chips, qc, hd, split, core_ref, gain_ref, wq_ref, wk_ref, wv_ref, mine_ref, theirs_ref):
    gain = diagonal(gain_ref)
    for out_ref, k in ((mine_ref, core_ref[0]), (theirs_ref, 1 - core_ref[0])):
        for i in range(chips):
            at = pl.ds(pl.multiple_of((2 * i + k) * qc, qc), qc)
            out_ref[:, i * qc : (i + 1) * qc] = mm(gain, wq_ref[:, at], 1, 0).astype(bf16)
            at = pl.ds(pl.multiple_of((2 * i + k if split else i) * hd, hd), hd)
            base = chips * qc + 2 * i * hd
            out_ref[:, base : base + hd] = mm(gain, wk_ref[:, at], 1, 0).astype(bf16)
            out_ref[:, base + hd : base + 2 * hd] = mm(gain, wv_ref[:, at], 1, 0).astype(bf16)


def small_call(kernel, scalars, args, outs, name):
    spec = lambda a: pl.BlockSpec(a.shape, lambda i, *_: (0,) * len(a.shape), pipeline_mode=pl.Buffered(1))
    size = lambda a: math.prod(a.shape) * a.dtype.itemsize
    return pl.pallas_call(
        kernel,
        grid_spec=pltpu.PrefetchScalarGridSpec(
            num_scalar_prefetch=1,
            grid=(1,),
            in_specs=[spec(a) for a in args],
            out_specs=[spec(o) for o in outs],
        ),
        out_shape=outs,
        cost_estimate=pl.CostEstimate(
            flops=0, bytes_accessed=sum(size(a) for a in (*args, *outs)), transcendentals=0
        ),
        compiler_params=pltpu.CompilerParams(vmem_limit_bytes=16 << 20),
        name=name,
    )(scalars, *args)


def select_qkv(core, gain, wq, wk, wv, chips, qc, hd, split):
    out = jax.ShapeDtypeStruct((wq.shape[0], chips * (qc + 2 * hd)), bf16)
    kernel = functools.partial(select_kernel, chips, qc, hd, split)
    return small_call(kernel, core[None], (gain, wq, wk, wv), (out, out), "select_qkv")


def select_units_kernel(chips, where_ref, gain_ref, wg_ref, wu_ref, mine_ref, theirs_ref):
    n = wg_ref.shape[1] // (4 * chips)
    gain = diagonal(gain_ref)
    for k in range(2):
        for z in range(2):

            @pl.when((where_ref[0] == k) & (where_ref[1] == z))
            def _():
                for out_ref, kk in ((mine_ref, k), (theirs_ref, 1 - k)):
                    for m, w_ref in enumerate((wg_ref, wu_ref)):
                        cols = [w_ref[:, (4 * i + 2 * kk + z) * n : (4 * i + 2 * kk + z + 1) * n] for i in range(chips)]
                        out = mm(gain, jnp.concatenate(cols, axis=1), 1, 0)
                        out_ref[:, m * chips * n : (m + 1) * chips * n] = out.astype(bf16)


def select_units(where, gain, wg, wu, chips):
    out = jax.ShapeDtypeStruct((wg.shape[0], wg.shape[1] // 2), bf16)
    kernel = functools.partial(select_units_kernel, chips)
    return small_call(kernel, where, (gain, wg, wu), (out, out), "select_units")


def place_units_kernel(chips, where_ref, gain_ref, a_ref, b_ref, dg_ref, du_ref):
    dr = dg_ref.shape[0]
    n = dg_ref.shape[1] // (4 * chips)
    gain = diagonal(gain_ref)
    for k in range(2):
        for z in range(2):

            @pl.when((where_ref[0] == k) & (where_ref[1] == z))
            def _():
                for m, out_ref in enumerate((dg_ref, du_ref)):
                    for i in range(chips):
                        cols = []
                        for kk in range(2):
                            for zz in range(2):
                                ref = a_ref if zz == z else b_ref
                                top = 0 if kk == k else dr
                                at = (m * chips + i) * n
                                cols.append(ref[top : top + dr, at : at + n])
                        out_ref[:, 4 * i * n : 4 * (i + 1) * n] = mm(gain, jnp.concatenate(cols, axis=1), 1, 0)


def place_units(where, gain, a, b, chips):
    out = jax.ShapeDtypeStruct((a.shape[0] // 2, 2 * a.shape[1]), f32)
    kernel = functools.partial(place_units_kernel, chips)
    return small_call(kernel, where, (gain, a, b), (out, out), "place_units")


def feed_kernel(chip_ref, xa_ref, xb_ref, ua_ref, ub_ref, wgu_ref, parts, hid_ref, gug_ref, ng_ref, out_ref, wd_ref):
    n = wd_ref.shape[0]
    first = pl.program_id(0) == 0

    @pl.when(first)
    def _():
        rows = n // len(parts)
        for rel, part in enumerate(parts):
            wd_ref[pl.ds(pl.multiple_of((chip_ref[0] ^ rel) * rows, rows), rows), :] = part[...]

    wgu, wd = wgu_ref[...], wd_ref[...]
    gu = mm(jnp.where(first, xa_ref[...], xb_ref[...]), wgu, 1, 0)
    hg = mm(jnp.where(first, ua_ref[...], ub_ref[...]), wd, 1, 1)
    gate, upper = gu[:, :n], gu[:, n:]
    sig = 1.0 / (1.0 + jnp.exp(-gate))
    act = gate * sig
    hidden = (act * upper).astype(bf16)
    hid_ref[...] = hidden
    gg = (hg * upper * sig * (1.0 + gate * (1.0 - sig))).astype(bf16)
    ug = (hg * act).astype(bf16)
    gug_ref[:, :n] = gg
    gug_ref[:, n:] = ug
    ng_ref[...] = (mm(gg, wgu[:, :n], 1, 1) + mm(ug, wgu[:, n:], 1, 1)).astype(bf16)
    out_ref[...] = mm(hidden, wd, 1, 0).astype(bf16)


def feed(xs, us, wgu, wd_parts, chip, first, blocks, into=()):
    r, d = xs[0].shape
    n = wgu.shape[1] // 2
    row = pl.BlockSpec((r, d), lambda i, _: (i, 0))
    block = lambda cols: pl.BlockSpec((r, cols), lambda i, _: (i + first, 0))
    whole = lambda a: pl.BlockSpec(a.shape, lambda i, _: (0, 0), pipeline_mode=pl.Buffered(1))
    shape = lambda rows, cols: jax.ShapeDtypeStruct((rows, cols), bf16)
    args = (*xs, *us, wgu, *wd_parts)
    k = 1 + len(args)
    body = lambda *refs: feed_kernel(*refs[:6], refs[6:k], *refs[k + len(into) :])
    return pl.pallas_call(
        body,
        grid_spec=pltpu.PrefetchScalarGridSpec(
            num_scalar_prefetch=1,
            grid=(2,),
            in_specs=[whole(a) for a in args] + [pl.BlockSpec(memory_space=pl.ANY)] * len(into),
            out_specs=[block(n), block(2 * n), row, row],
            scratch_shapes=[pltpu.VMEM((n, d), bf16)],
        ),
        out_shape=[shape(blocks * r, n), shape(blocks * r, 2 * n)] + [shape(2 * r, d)] * 2,
        input_output_aliases={k + i: i for i in range(len(into))},
        cost_estimate=pl.CostEstimate(
            flops=28 * r * d * n, bytes_accessed=2 * (8 * r * d + 6 * r * n + 3 * d * n), transcendentals=2 * r * n
        ),
        name="feed",
    )(chip[None], *args, *into)


def after(x, *deps):
    return lax.optimization_barrier((x, *deps))[0]


def row_norm(values):
    scale = lax.rsqrt(jnp.mean(values * values, axis=-1, keepdims=True) + EPS)
    return (values * scale).astype(bf16), scale


def row_norm_back(values, scale, weighted):
    inner = jnp.mean(weighted * values, axis=-1, keepdims=True)
    return scale * weighted - values * (scale * scale * scale * inner)


def build(mesh):
    F, Z = mesh.shape["fsdp"], mesh.shape["ctx"]
    C = F // 2
    assert F == 2 * C and F & (F - 1) == 0 and Z & (Z - 1) == 0 and Z > 1
    chip_bits = [2 << i for i in range(C.bit_length() - 1)]
    z_bits = [1 << i for i in range(Z.bit_length() - 1)]
    sizes = {"fsdp": F, "ctx": Z}

    def hop(x, axis, bit):
        return lax.ppermute(x, axis, [(i, i ^ bit) for i in range(sizes[axis])])

    def shift(x, by):
        return lax.ppermute(x, "ctx", [(i, i + by) for i in range(Z) if 0 <= i + by < Z])

    def place(buf, part, c, rel):
        return lax.dynamic_update_slice(buf, part, ((c ^ rel) * (buf.shape[0] // C), 0))

    def by_chip(parts, c, *deps):
        r, n = parts[0].shape
        out = after(jnp.zeros((C * r, n), parts[0].dtype), *deps)
        for rel, part in enumerate(parts):
            out = place(out, part, c, rel)
        return out

    def spread(piece):
        return [piece] + [hop(piece, "fsdp", 2 * rel) for rel in range(1, C)]

    def by_chip_copies(piece):
        return jnp.broadcast_to(piece, (C, *piece.shape))

    def exchange(copies):
        out = lax.all_to_all(copies, "fsdp", 0, 0, axis_index_groups=groups)
        return out.reshape(-1, out.shape[-1])

    groups = [[2 * i + k for i in range(C)] for k in range(2)]

    def scatter(full):
        full = full.reshape(C, -1, full.shape[-1])
        return lax.all_to_all(full, "fsdp", 0, 0, axis_index_groups=groups)

    def scatter_hops(full, c):
        r = full.shape[0] // C
        parts = [lax.dynamic_slice_in_dim(full, (c ^ rel) * r, r) for rel in range(C)]
        return [parts[0]] + [hop(parts[rel], "fsdp", 2 * rel) for rel in range(1, C)]

    def total(parts, *deps):
        if not isinstance(parts, list):
            return jnp.sum(after(parts, *deps).astype(f32), axis=0)
        return functools.reduce(lambda a, b: a + b, [after(p, *deps).astype(f32) for p in parts])

    def z_sum(b, bits):
        for bit in bits:
            b = (b.astype(f32) + hop(b, "ctx", bit).astype(f32)).astype(bf16)
        return b

    def z_sum_split(own, zb):
        h = own.shape[0] // 2
        top, bottom = own[:h], own[h:]
        mine, theirs = jnp.where(zb == 0, top, bottom), jnp.where(zb == 0, bottom, top)
        mine = mine.astype(f32) + hop(theirs.astype(bf16), "ctx", 1).astype(f32)
        b = z_sum(mine.astype(bf16), z_bits[1:])
        o = hop(b, "ctx", 1)
        return jnp.where(zb == 0, jnp.concatenate([b, o]), jnp.concatenate([o, b]))

    def body(
        tokens, segments, cotangent, attn_gain, w_query, key_matrix, value_matrix, w_out,
        query_gain, key_gain, ffn_gain, w_gate, w_up, w_down,
    ):
        me = lax.axis_index("fsdp")
        core, c = me % 2, me // 2
        zb = lax.axis_index("ctx") % 2
        R, D = tokens.shape[1:]
        hd = query_gain.shape[0]
        heads, kv_heads = w_query.shape[1] // hd, key_matrix.shape[1] // hd
        group = heads // F
        kv_split = kv_heads == F
        assert heads % F == 0 and (kv_split or (kv_heads == C and heads == F))
        halos = -(-(DOC_MAX - 1) // R)
        K = (halos + 1) * R
        qc = group * hd
        dr = w_query.shape[0]
        FS = w_down.shape[0] // 2
        swap = lambda x: hop(x, "fsdp", 1)
        by_core = lambda a, b: jnp.where(core == 0, a, b)

        where = jnp.stack([core, zb])

        def chip_rows(mine, theirs):
            got = swap(theirs)
            return by_core(jnp.concatenate([mine, got]), jnp.concatenate([got, mine]))

        mine, theirs = select_qkv(core, attn_gain[None], w_query, key_matrix, value_matrix, C, qc, hd, kv_split)
        qkv_piece = by_chip_copies(chip_rows(mine, theirs))
        qkv = exchange(qkv_piece)
        pad = 16
        seg_rows = jnp.zeros((pad, D), bf16).at[0, :R].set((segments[0] + 1).astype(bf16))
        cur = jnp.concatenate([tokens[0], seg_rows])

        gu_piece = chip_rows(*select_units(where, ffn_gain[None], after(w_gate, qkv_piece), w_up, C))
        gu_copies = by_chip_copies(gu_piece)
        d_w = after(w_down, gu_piece)
        d_piece = jnp.where(zb == 0, d_w[:FS], d_w[FS:])
        cur = after(cur, qkv_piece)
        window = [shift(cur, i) for i in range(halos, 0, -1)] + [cur]
        half = hd // 2
        freq = 1.0 / ROPE_BASE ** (jnp.arange(half, dtype=f32) * 2.0 / hd)
        angle = after(jnp.arange(K, dtype=f32), qkv_piece)[:, None] * freq[None, :]
        cosine, sine = jnp.cos(angle), jnp.sin(angle)
        window = jnp.stack(window)
        window = jnp.stack([window, swap(window)])
        seg = window[:, :, R, :R].reshape(2, K).astype(jnp.int32)
        toks = window[:, :, :R].reshape(2, K, D)
        tables = (
            jnp.concatenate([cosine, cosine], axis=1),
            jnp.concatenate([-sine, sine], axis=1),
            seg[:, K - R :, None],
            seg[:, None, :],
            query_gain.astype(f32)[None],
            key_gain.astype(f32)[None],
        )
        normed, scale_attn = row_norm(after(toks, gu_copies, tables[0], tables[1], d_piece).astype(f32))

        qkv, normed = lax.optimization_barrier((qkv, normed))
        o_parts = spread(after(w_out, qkv))

        wq, wkv = qkv[:, : C * qc], qkv[:, C * qc :]
        normed_own = normed[:, K - R :].reshape(2 * R, D)
        normed_all = normed.reshape(2 * K, D)
        kv_raw = mm(normed_all, wkv, 1, 0)
        q_raw = mm(normed_own, wq, 1, 0)
        w_gu = exchange(after(gu_copies, qkv))
        d_parts = spread(after(d_piece, qkv))
        context = attend(q_raw, after(kv_raw, q_raw), tables, 2, R, K, group, hd)
        cot = after(cotangent[0], q_raw)
        cot_z = hop(cot, "ctx", 1)
        us = [cot, swap(cot), cot_z, swap(cot_z)]
        w_o = by_chip([after(p, context) for p in o_parts], c)
        part = mm(context, w_o, 1, 0)
        middle = toks[0, K - R :].astype(f32) + part[:R] + swap(part[R:].astype(bf16)).astype(f32)

        nf, scale_ffn = row_norm(middle)
        nf_z = hop(after(nf, w_gu), "ctx", 1)
        xs = [nf, swap(nf)]
        hidden, gug, ng_own, out_own = feed(xs, us[:2], w_gu, d_parts, c, 0, 4)
        xs += [nf_z, swap(after(nf_z, ng_own))]
        hidden, gug, ng_z, out_z = feed(xs[2:], us[2:], w_gu, d_parts, c, 2, 4, (hidden, gug))
        x4, u4 = jnp.concatenate(xs), jnp.concatenate(us)

        ng_send = (ng_z[:R].astype(f32) + swap(ng_z[R:]).astype(f32)).astype(bf16)
        ng_got = hop(ng_send, "ctx", 1)
        ng_here = ng_own[:R].astype(f32) + swap(ng_own[R:]).astype(f32)

        gu_grads = scatter(mm(after(x4, ng_send), gug, 0, 0).astype(bf16))
        down_full = mm(after(hidden, ng_send), u4, 0, 0).astype(bf16)

        normed_grad = ng_here + after(ng_got, down_full).astype(f32)
        ffn_gain_term = jnp.sum(normed_grad * middle * scale_ffn, axis=0)
        middle_grad = cotangent[0].astype(f32) + row_norm_back(middle, scale_ffn, normed_grad)

        ml = middle_grad.astype(bf16)
        ml2 = jnp.concatenate([ml, swap(ml)])
        out_send = (out_z[:R].astype(f32) + swap(after(out_z[R:], ml)).astype(f32)).astype(bf16)
        out_here = out_own[:R].astype(f32) + swap(out_own[R:]).astype(f32)
        out_got = hop(out_send, "ctx", 1)
        context_grad = mm(ml2, w_o, 1, 1).astype(bf16)
        out_full = mm(context, after(ml2, context_grad), 0, 0).astype(bf16)
        down_out = jnp.concatenate([down_full.reshape(C, -1, D), out_full.reshape(C, -1, D)], axis=1).reshape(-1, D)
        do_grads = scatter_hops(down_out, c)

        def core_rows(rows):
            top, bottom = rows[:dr], rows[dr:]
            mine, theirs = by_core(top, bottom), by_core(bottom, top)
            return mine, swap(theirs.astype(bf16)).astype(f32)

        def by_parity(mine, other):
            return by_core(mine, other), by_core(other, mine)

        cg = after(context_grad, out_send, down_out)
        dq, dkv, qgg, kgg = attend_back(q_raw, kv_raw, cg, tables, 2, R, K, group, hd)
        gu_grads = after(gu_grads, dq)
        mine, got = core_rows(total(gu_grads))
        gu_s = jnp.concatenate([mine, got]).astype(bf16)
        gu_z = z_sum(gu_s, z_bits[1:])

        q_full = mm(normed_own, after(dq, gu_s), 0, 0).astype(bf16)
        kv_full = mm(normed_all, after(dkv, gu_s), 0, 0).astype(bf16)
        qkv_grads = scatter(jnp.concatenate([q_full, kv_full], axis=1))

        do_sum = total(do_grads, q_full, kv_full, gu_z)
        zpick = lambda x: (jnp.where(zb == 0, x[0], x[1]), jnp.where(zb == 0, x[1], x[0]))
        mine, theirs = zpick(do_sum[FS:].reshape(2, -1, D))
        mine = mine + hop(theirs.astype(bf16), "ctx", 1).astype(f32)
        do_s = jnp.concatenate([do_sum[:FS], mine]).astype(bf16)
        do_z = z_sum(do_s, z_bits[1:])
        do_o = hop(do_z, "ctx", 1)
        o = hop(gu_z, "ctx", 1)

        sent = (do_s,)
        own_rows = mm(after(dq, *sent), wq, 1, 1)
        attn_grad = mm(after(dkv, *sent), wkv, 1, 1).reshape(2, K, D)
        attn_grad = attn_grad + jnp.pad(own_rows.reshape(2, R, D), ((0, 0), (K - R, 0), (0, 0)))
        attn_grad = attn_grad[0] + swap(after(attn_grad[1].astype(bf16), qkv_grads)).astype(f32)
        attn_gain_term = jnp.sum(attn_grad * toks[0].astype(f32) * scale_attn[0], axis=0)
        carry = attn_grad[:R]
        for i in range(1, halos + 1):
            carry = attn_grad[i * R : (i + 1) * R] + shift(carry.astype(bf16), -1).astype(f32)
        input_grad = middle_grad + row_norm_back(
            toks[0, K - R :].astype(f32), scale_attn[0, K - R :], carry
        )

        small = jnp.concatenate([qgg[0], kgg[0], ffn_gain_term, attn_gain_term])
        small = small.reshape(-1, 128)
        small = small + swap(small)
        small = functools.reduce(lambda a, b: a + b, [small] + [hop(small, "fsdp", 2 * rel) for rel in range(1, C)])
        small = small.reshape(-1)
        own = lambda base: lax.dynamic_slice_in_dim(small, base + me * dr, dr)
        gains = jnp.concatenate([own(2 * hd), own(2 * hd + D), small[: 2 * hd]]).reshape(-1, 128)
        for bit in z_bits:
            gains = gains + hop(gains, "ctx", bit)
        gains = gains.reshape(-1)

        attn_rows = attn_gain.astype(f32)[:, None]
        d_gate, d_up = place_units(where, ffn_gain[None], gu_z, o, C)
        output = (middle + out_here + after(out_got, dq).astype(f32)).astype(bf16)

        mine, got = core_rows(total(qkv_grads))
        nq = C * qc
        rows = [mine[:, :nq], got[:, :nq]]
        if kv_split:
            rows += [mine[:, nq:], got[:, nq:]]
        full = z_sum_split(jnp.concatenate(rows), zb).astype(f32)
        rows = [full[i * dr : (i + 1) * dr] * attn_rows for i in range(len(rows))]
        pair = by_parity(*rows[:2])
        d_query = jnp.concatenate([p[:, i * qc : (i + 1) * qc] for i in range(C) for p in pair], axis=1)
        if kv_split:
            kv = by_parity(*rows[2:])
        else:
            kv = (z_sum_split(mine[:, nq:] + got[:, nq:], zb).astype(f32) * attn_rows,)
        pick = lambda off: jnp.concatenate(
            [p[:, 2 * i * hd + off : 2 * i * hd + off + hd] for i in range(C) for p in kv], axis=1
        )
        d_key, d_value = pick(0), pick(hd)

        both = [jnp.where(zb == 0, do_z, do_o), jnp.where(zb == 0, do_o, do_z)]
        d_down = jnp.concatenate([b[:FS] for b in both]).astype(f32)
        d_out = jnp.concatenate([b[FS:] for b in both]).astype(f32)
        d_ffn_gain = gains[:dr] / ffn_gain.astype(f32)
        d_attn_gain = gains[dr : 2 * dr] / attn_gain.astype(f32)
        head_gains = gains[2 * dr : 2 * dr + 2 * hd]
        return (
            output[None],
            input_grad[None],
            d_attn_gain,
            d_query,
            d_key,
            d_value,
            d_out,
            head_gains[:hd],
            head_gains[hd:],
            d_ffn_gain,
            d_gate,
            d_up,
            d_down,
        )

    return body


def solution(mesh):
    row = P("fsdp", None)
    token = P("fsdp", "ctx", None)
    in_specs = (token, P("fsdp", "ctx"), token, P("fsdp"), row, row, row, row, P(), P(), P("fsdp"), row, row, row)
    out_specs = (token, token, P("fsdp"), row, row, row, row, P(), P(), P("fsdp"), row, row, row)
    return jax.shard_map(build(mesh), mesh=mesh, in_specs=in_specs, out_specs=out_specs, check_vma=False)
```
